256 devices in a mesh: cp: 64 (over y_lo, x, z), tp: 4 (over y_hi, core).
Axes of the slice: x: 4, y: 4 (y_hi: 2, y_lo: 2; y = y_hi * 2 + y_lo), z: 8, core: 2. Of those that a mesh axis runs over, the one named last changes fastest.
Arguments:
- queries: bfloat16 [12288, 2048], P('cp', 'tp'), may hold values from -128 to 128
- keys: bfloat16 [12288, 256], P('cp'), may hold values from -6 to 6
- values: bfloat16 [12288, 256], P('cp'), may hold values from -6 to 6
- positions: int32 [12288], replicated, may hold values from 0 to 12287, as said below
- out_weight: bfloat16 [2048, 8192], P('tp'), may hold values from -0.125 to 0.125
Outputs:
- mixed: bfloat16 [12288, 8192], P(('cp', 'tp'))
The draws below stay inside these ranges and needn't reach their ends.
Inputs may be any that keep to these rules, and one draw needn't show every extreme that they name: positions is a permutation of 0 to 12287. The tokens stored at indices d * 192 to (d + 1) * 192 - 1 form two runs of 96 consecutive positions, the first starting at b * 96 and the second at (127 - b) * 96 for some b, each b used by one d.
All inputs are finite; a program needn't handle non-finite values.
Results may differ from the reference program's by a relative error of at most 0.013.
Values may be sent and summed in bfloat16 or wider, within the bound.
A program may use at most 128 MiB of HBM per device.

```python
import math
import jax
import jax.numpy as jnp
from jax import lax

D = 8192
HEAD = 128
GROUP = 8
KV = 2
TOK_DEV = 192
H = 16
TOKENS = 12288
N_TP = 4


def joint_draw(key):
    seed_base = jax.random.fold_in(key, 11)
    seed_query, seed_keys = jax.random.split(seed_base, 2)
    queries = jnp.clip(jax.random.normal(seed_query, (TOKENS, GROUP * KV * HEAD), jnp.float32), -6.0, 6.0)
    keys = jnp.clip(jax.random.normal(seed_keys, (TOKENS, KV * HEAD), jnp.float32), -6.0, 6.0)
    return (queries, keys)


def draw_queries(key, part):
    return joint_draw(key)[0].astype(jnp.bfloat16)


def draw_keys(key, part):
    return joint_draw(key)[1].astype(jnp.bfloat16)


def draw_positions(key, part):
    slot_count = TOKENS // TOK_DEV
    half_rows = TOK_DEV // 2
    slot_order = jax.random.permutation(jax.random.fold_in(key, 5), slot_count)
    block_start = jnp.stack([slot_order, 2 * slot_count - 1 - slot_order], axis=1)
    position = block_start[:, :, None] * half_rows + jnp.arange(half_rows)[None, None, :]
    return position.reshape(-1).astype(jnp.int32)


def block_levels(own_key, extent, shards, smallest, top_value):
    gain, own = 1.0, jax.random.fold_in(own_key, 6)
    for axis_at, parts in shards:
        heights = jnp.exp(jax.random.uniform(jax.random.fold_in(own, axis_at), (parts,), jnp.float32, smallest / len(shards), top_value / len(shards)))
        gain = gain * jnp.repeat(heights, extent[axis_at] // parts).reshape([-1 if axis == axis_at else 1 for axis in range(len(extent))])
    return gain


def bell_draw(own_key, extent, spread, most, cuts=(), kind=jnp.bfloat16):
    level = block_levels(own_key, extent, cuts, -0.22, 0.18) if cuts else 1.0
    entries = jax.random.normal(own_key, extent, jnp.float32) * spread * level
    return jnp.minimum(jnp.maximum(entries, -most), most).astype(kind)


def setup_inputs(seed: int = 0) -> dict:
    splits = jax.random.split(jax.random.key(seed), 6)
    queries = draw_queries(jax.random.fold_in(splits[5], 71), 0)
    keys = draw_keys(jax.random.fold_in(splits[5], 71), 0)
    values = bell_draw(splits[2], (TOKENS, KV * HEAD), 1.0, 6.0, ((0, 64),))
    positions = draw_positions(jax.random.fold_in(splits[5], 71), 0)
    out_weight = bell_draw(splits[4], (H * HEAD, D), (H * HEAD) ** -0.5, 0.125, ((0, 4),))
    return dict(queries=queries, keys=keys, values=values, positions=positions, out_weight=out_weight)


def reference(queries, keys, values, positions, out_weight):
    token_count = queries.shape[0]
    head_count = queries.shape[1] // HEAD
    score_scale = HEAD ** -0.5
    block_rows = math.gcd(token_count, 512)

    def one_block(block_index):
        first = (block_index * block_rows).astype(jnp.int32)
        query_block = lax.dynamic_slice_in_dim(queries, first, block_rows, 0)
        query_pos = lax.dynamic_slice_in_dim(positions, first, block_rows, 0)
        allowed = positions[None, :] <= query_pos[:, None]

        def one_head(head_index):
            kv_group = head_index // GROUP
            query_head = lax.dynamic_slice_in_dim(query_block, (head_index * HEAD).astype(jnp.int32), HEAD, 1)
            key_head = lax.dynamic_slice_in_dim(keys, (kv_group * HEAD).astype(jnp.int32), HEAD, 1)
            value_head = lax.dynamic_slice_in_dim(values, (kv_group * HEAD).astype(jnp.int32), HEAD, 1)
            scores = jnp.dot(query_head, key_head.T, preferred_element_type=jnp.float32) * score_scale
            scores = jnp.where(allowed, scores, -1e30)
            row_max = jnp.max(scores, axis=1, keepdims=True)
            weights = jnp.where(allowed, jnp.exp(scores - row_max), 0.0)
            row_sum = jnp.sum(weights, axis=1, keepdims=True)
            head_out = jnp.dot(weights.astype(jnp.bfloat16), value_head, preferred_element_type=jnp.float32) / row_sum
            return head_out.astype(jnp.bfloat16)

        stacked = lax.map(one_head, jnp.arange(head_count, dtype=jnp.int32))
        return jnp.transpose(stacked, (1, 0, 2)).reshape(block_rows, head_count * HEAD)

    attended = lax.map(one_block, jnp.arange(token_count // block_rows, dtype=jnp.int32))
    attended = attended.reshape(token_count, head_count * HEAD)
    slab_width = attended.shape[1] // N_TP
    mixed = jnp.zeros((token_count, out_weight.shape[1]), jnp.float32)
    for slab in range(N_TP):
        partial_sum = jnp.dot(attended[:, slab * slab_width:(slab + 1) * slab_width],
                              out_weight[slab * slab_width:(slab + 1) * slab_width],
                              preferred_element_type=jnp.float32).astype(jnp.bfloat16)
        partial_sum = lax.optimization_barrier(partial_sum)
        mixed = mixed + partial_sum.astype(jnp.float32)
    return mixed.astype(jnp.bfloat16)
```

```python
import functools
import math

import jax
import jax.numpy as jnp
from jax import lax
from jax.experimental import pallas as pl
from jax.experimental.pallas import tpu as pltpu
from jax.sharding import PartitionSpec as P

MESH = pl.DeviceIdType.MESH
HEAD = 128
GROUP = 8
NY, NX, NZ = 2, 4, 8
NCP = NY * NX * NZ
RUN = 96
TOK = 192
HEADS = 4
ROWS = RUN * HEADS
NCOL = 8192
HALF = NCOL // 2
NJ = 8
CW = HALF // NJ
SCALE = HEAD ** (-0.5) * math.log2(math.e)
NEG = -1e30


def kernel(q_ref, k_ref, v_ref, pos_ref, w_ref, out_ref,
           kv, own_kv, qv, q2t, acc_l, acc_h, sum_l, sum_h, max_l, max_h,
           att, wbuf, pbuf, relay, rbuf, lbuf, obuf, pos,
           fill_sem, in_sem, w_sem, ag_send, ag_recv, dd_send, dd_recv,
           att_sem, rs_send, rs_recv, fw_send, fw_recv, lo_send, lo_recv, out_sem):
    cp = lax.axis_index("cp")
    tp = lax.axis_index("tp")
    core = tp % 2
    yh = tp // 2
    z = cp % NZ
    x = (cp // NZ) % NX
    y = cp // (NZ * NX)

    def cp_of(yy, xx, zz):
        return (yy * NX + xx) * NZ + zz

    partner = dict(cp=cp, tp=yh * 2 + 1 - core)

    def at_z(k):
        return dict(cp=cp_of(y, x, (z + k + NZ) % NZ), tp=tp)

    def at_x(k):
        return dict(cp=cp_of(y, (x + k + NX) % NX, z), tp=tp)

    flip = dict(cp=cp_of(1 - y, x, z), tp=tp)

    def ring_y(sign, e):
        yy = (yh * 2 + y + sign + 4) % 4
        return dict(cp=cp_of(yy % 2, x, z), tp=(yy // 2) * 2 + e)

    q_copy = pltpu.make_async_copy(q_ref, qv, in_sem.at[0])
    q_copy.start()
    pos_copy = pltpu.make_async_copy(pos_ref, pos, in_sem.at[1])
    pos_copy.start()
    slot_a = z * 8 + x * 2 + y
    slot_b = x * 16 + z * 2 + y
    slot_d = y * 32 + x * 8 + z
    own_slots = (slot_a, slot_b, slot_d)
    fills = []
    cols = pl.ds(pl.multiple_of(yh * HEAD, HEAD), HEAD)
    for f in range(3):
        for h in range(2):
            for src, kind in ((k_ref, 0), (v_ref, 2)):
                rows = pl.ds(pl.multiple_of(h * RUN + 32 * f + 16 * core, 16), 16)
                fills.append(pltpu.make_async_copy(
                    src.at[rows, cols], kv.at[f, core, own_slots[f], kind + h], fill_sem.at[len(fills)]))
    own_fills = []
    for h in range(2):
        for src, kind in ((k_ref, 0), (v_ref, 2)):
            own_fills.append(pltpu.make_async_copy(
                src.at[pl.ds(h * RUN, RUN), cols], own_kv.at[kind + h], fill_sem.at[12 + len(own_fills)]))
    for c in fills + own_fills:
        c.start()

    barrier = pltpu.get_barrier_semaphore()
    peers = [at_z(k) for k in range(1, NZ)] + [at_x(k) for k in range(1, NX)] + [partner]
    peers += [ring_y(s, e) for s in (1, -1) for e in (0, 1)]
    for p in peers:
        pl.semaphore_signal(barrier, inc=1, device_id=p, device_id_type=MESH)
    pl.semaphore_wait(barrier, len(peers))
    for c in fills:
        c.wait()

    sends = []

    def rcopy(src, dst, ssem, rsem, dev):
        return pltpu.make_async_remote_copy(src_ref=src, dst_ref=dst, send_sem=ssem, recv_sem=rsem,
                                            device_id=dev, device_id_type=MESH)

    def gather(f, slot, n, sem, dev):
        ref = kv.at[f, core, pl.ds(slot, n)]
        c = rcopy(ref, ref, ag_send.at[sem], ag_recv.at[sem], dev)
        c.start()
        sends.append(c)

    def arrive(f, slot, n, sem):
        ref = kv.at[f, core, pl.ds(slot, n)]
        rcopy(ref, ref, ag_send.at[sem], ag_recv.at[sem], partner).wait_recv()

    def share(f, slot, n, sem):
        ref = kv.at[f, core, pl.ds(slot, n)]
        c = rcopy(ref, ref, dd_send.at[sem], dd_recv.at[sem], partner)
        c.start()
        sends.append(c)

    def shared(f, slot, n, sem):
        ref = kv.at[f, 1 - core, pl.ds(slot, n)]
        rcopy(ref, ref, dd_send.at[sem], dd_recv.at[sem], partner).wait_recv()

    def zz(k):
        return (z + k + NZ) % NZ

    def xx(k):
        return (x + k + NX) % NX

    sem_ids = {}

    def sid(*key):
        return sem_ids.setdefault(key, len(sem_ids))

    gather(0, slot_a, 1, sid("a.y"), flip)
    gather(1, slot_b, 1, sid("b.y"), flip)
    for k in (1, -1, 2, -2, 3, -3, 4):
        gather(2, slot_d, 1, sid("d.z", -k if k != 4 else 4), at_z(k))

    my_rows = pl.ds(pl.multiple_of(core * 512, 512), 512)
    w_own = pltpu.make_async_copy(
        w_ref.at[:, pl.ds(pl.multiple_of(core * HALF, HALF), HALF)], wbuf.at[my_rows], w_sem.at[0])
    w_own.start()
    w_far = rcopy(w_ref.at[:, pl.ds(pl.multiple_of((1 - core) * HALF, HALF), HALF)], wbuf.at[my_rows],
                  w_sem.at[1], w_sem.at[2], partner)
    w_far.start()
    other_rows = pl.ds(pl.multiple_of((1 - core) * 512, 512), 512)
    w_in = rcopy(w_ref.at[:, pl.ds(0, HALF)], wbuf.at[other_rows], w_sem.at[1], w_sem.at[2], partner)

    arrive(0, z * 8 + x * 2 + 1 - y, 1, sid("a.y"))
    for k in (1, -1, 2):
        gather(0, z * 8 + x * 2, 2, sid("a.x", -k if k != 2 else 2), at_x(k))
    arrive(1, x * 16 + z * 2 + 1 - y, 1, sid("b.y"))

    def send_b_z(k, sign):
        gather(1, x * 16 + zz(-sign * k) * 2, 2, sid("b.z", sign, k + 1), at_z(sign))

    def send_b_x(k):
        slot = x * 16 + zz(k) * 2
        gather(1, slot, 2, sid("b.x", k % NZ, 1), at_x(1))
        gather(1, slot, 2, sid("b.x", k % NZ, -1), at_x(-1))

    def relay_b_x(k):
        zk = zz(k)
        arrive(1, xx(-1) * 16 + zk * 2, 2, sid("b.x", k % NZ, 1))
        if k % 2 == 0:
            gather(1, xx(-1) * 16 + zk * 2, 2, sid("b.x", k % NZ, 2), at_x(1))
        arrive(1, xx(1) * 16 + zk * 2, 2, sid("b.x", k % NZ, -1))
        if k % 2 == 1:
            gather(1, xx(1) * 16 + zk * 2, 2, sid("b.x", k % NZ, 2), at_x(-1))

    def last_b_x(k):
        arrive(1, xx(2) * 16 + zz(k) * 2, 2, sid("b.x", k % NZ, 2))

    def arrive_b_z(k, sign):
        arrive(1, x * 16 + zz(-sign * k) * 2, 2, sid("b.z", sign, k))

    STEPS = {1: 4, -1: 3}

    send_b_z(0, 1)
    send_b_z(0, -1)
    send_b_x(0)

    for k in (1, -1, 2):
        arrive(0, z * 8 + xx(k) * 2, 2, sid("a.x", k))
    A_STEPS = {(0, 1): 4, (0, -1): 3, (1, 1): 3, (1, -1): 4}

    def send_a_z(k, sign, piece):
        gather(0, zz(-sign * k) * 8 + piece * 4, 4, sid("a.z", piece, sign, k + 1), at_z(sign))

    def arrive_a_z(k, sign, piece):
        arrive(0, zz(-sign * k) * 8 + piece * 4, 4, sid("a.z", piece, sign, k))

    for piece in (0, 1):
        for sign in (1, -1):
            send_a_z(0, sign, piece)
    share(0, z * 8, 8, 0)

    for k in (1, -1, 2, -2, 3, -3, 4):
        arrive(2, y * 32 + x * 8 + zz(k), 1, sid("d.z", k))
    own_line = y * 32 + x * 8
    gather(2, own_line, 8, sid("d.x", 1), at_x(1))
    gather(2, own_line, 8, sid("d.x", -1), at_x(-1))
    gather(2, own_line, 8, sid("d.y", 0), flip)
    share(2, own_line, 8, 16)

    def flow_a(k):
        for piece in (0, 1):
            for sign in (1, -1):
                last = A_STEPS[piece, sign]
                if k <= last:
                    arrive_a_z(k, sign, piece)
                    if k < last:
                        send_a_z(k, sign, piece)
        if k < 4:
            share(0, zz(k) * 8, 8, k)
            share(0, zz(-k) * 8, 8, 8 - k)
        else:
            share(0, zz(4) * 8, 8, 4)

    def flow_b(k):
        for sign in (1, -1):
            if k <= STEPS[sign]:
                arrive_b_z(k, sign)
                if k < STEPS[sign]:
                    send_b_z(k, sign)
                send_b_x(-sign * k)

    flow_b(1)
    relay_b_x(0)
    flow_a(1)
    flow_b(2)
    relay_b_x(1)
    relay_b_x(-1)
    arrive(2, y * 32 + xx(-1) * 8, 8, sid("d.x", 1))
    gather(2, y * 32 + xx(-1) * 8, 4, sid("d.x2", 0), at_x(1))
    gather(2, y * 32 + xx(-1) * 8, 8, sid("d.y", -1), flip)
    share(2, y * 32 + xx(-1) * 8, 8, 17)
    arrive(2, y * 32 + xx(1) * 8, 8, sid("d.x", -1))
    gather(2, y * 32 + xx(1) * 8 + 4, 4, sid("d.x2", 1), at_x(-1))
    gather(2, y * 32 + xx(1) * 8, 8, sid("d.y", 1), flip)
    share(2, y * 32 + xx(1) * 8, 8, 18)
    flow_a(2)
    flow_b(3)
    relay_b_x(2)
    relay_b_x(-2)
    arrive(2, y * 32 + xx(2) * 8, 4, sid("d.x2", 0))
    arrive(2, y * 32 + xx(2) * 8 + 4, 4, sid("d.x2", 1))
    gather(2, y * 32 + xx(2) * 8, 8, sid("d.y", 2), flip)
    share(2, y * 32 + xx(2) * 8, 8, 19)
    flow_b(4)
    share(1, x * 16, 16, 8)
    flow_a(3)
    relay_b_x(3)
    relay_b_x(-3)
    relay_b_x(4)
    share(1, xx(-1) * 16, 16, 9)
    share(1, xx(1) * 16, 16, 10)
    arrive(2, (1 - y) * 32 + x * 8, 8, sid("d.y", 0))
    share(2, (1 - y) * 32 + x * 8, 8, 20)
    for k in (-1, 1):
        arrive(2, (1 - y) * 32 + xx(k) * 8, 8, sid("d.y", k))
        share(2, (1 - y) * 32 + xx(k) * 8, 8, 22 + k)
    flow_a(4)
    for k in (0, 1, -1, 2, -2, 3, -3, 4):
        last_b_x(k)
    share(1, xx(2) * 16, 16, 11)
    arrive(2, (1 - y) * 32 + xx(2) * 8, 8, sid("d.y", 2))
    share(2, (1 - y) * 32 + xx(2) * 8, 8, 22)

    assert len(sem_ids) == N_AG

    q_copy.wait()
    pos_copy.wait()
    own0 = pos[cp * TOK]
    own1 = pos[cp * TOK + RUN]
    own_first = own0 < own1
    own_low = jnp.minimum(own0, own1)

    qa = jnp.concatenate([qv[0:RUN, h * HEAD:(h + 1) * HEAD] for h in range(HEADS)], axis=0)
    qb = jnp.concatenate([qv[RUN:TOK, h * HEAD:(h + 1) * HEAD] for h in range(HEADS)], axis=0)
    q2t[0:HEAD, :] = jnp.where(own_first, qa, qb).T
    q2t[HEAD:2 * HEAD, :] = jnp.where(own_first, qb, qa).T

    TN = (((0,), (0,)), ((), ()))

    for c in own_fills:
        c.wait()

    lane = lax.broadcasted_iota(jnp.int32, (RUN, ROWS), 1)
    keep = lax.broadcasted_iota(jnp.int32, (RUN, ROWS), 0) <= lane % RUN

    def triangle(kk, vv, qt, acc, total, top):
        s = jnp.dot(kk, qt, preferred_element_type=jnp.float32)
        s = jnp.where(keep, s, NEG)
        m = jnp.max(s, axis=0, keepdims=True)
        p = jnp.exp2(s * SCALE - m * SCALE)
        top[...] = m
        total[...] = jnp.sum(p.reshape(RUN // 8, 8, ROWS), axis=0)
        acc[...] = lax.dot_general(vv, p.astype(jnp.bfloat16), TN, preferred_element_type=jnp.float32)

    k0, k1, v0, v1 = (own_kv[i] for i in range(4))
    triangle(jnp.where(own_first, k0, k1), jnp.where(own_first, v0, v1), q2t[0:HEAD, :], acc_l, sum_l, max_l)
    triangle(jnp.where(own_first, k1, k0), jnp.where(own_first, v1, v0), q2t[HEAD:2 * HEAD, :], acc_h, sum_h, max_h)

    zero = jnp.zeros((16, HEAD), jnp.bfloat16)

    def chunk(f, i):
        low_f, high_f = [], []
        kl, vl, ka, kb, va, vb = [], [], [], [], [], []
        for j in range(8):
            s_z = jnp.where(f == 0, i, jnp.where(f == 1, (i % 2) * 4 + j // 2, j))
            s_x = jnp.where(f == 0, j // 2, jnp.where(f == 1, i // 2, i % 4))
            s_y = jnp.where(f == 2, i // 4, j % 2)
            s = cp_of(s_y, s_x, s_z)
            p0 = pos[s * TOK]
            p1 = pos[s * TOK + RUN]
            first = p0 < p1
            low = jnp.minimum(p0, p1) < own_low
            high = jnp.minimum(p0, p1) > own_low
            low_f.append(low)
            high_f.append(high)
            for c in range(2):
                t0, t1, u0, u1 = (kv[f, c, i * 8 + j, n] for n in range(4))
                kl_ = jnp.where(first, t0, t1)
                vl_ = jnp.where(first, u0, u1)
                kl.append(kl_)
                vl.append(vl_)
                ka.append(jnp.where(low, kl_, zero))
                va.append(jnp.where(low, vl_, zero))
                kb.append(jnp.where(high, jnp.where(first, t1, t0), zero))
                vb.append(jnp.where(high, jnp.where(first, u1, u0), zero))
        cat = functools.partial(jnp.concatenate, axis=0)
        k2 = jnp.concatenate([cat(ka), cat(kb)], axis=1)
        v2 = jnp.concatenate([cat(va), cat(vb)], axis=1)
        s1 = jnp.dot(cat(kl), q2t[HEAD:2 * HEAD, :], preferred_element_type=jnp.float32)
        s2 = jnp.dot(k2, q2t[...], preferred_element_type=jnp.float32)
        m_h = jnp.max(s1.reshape(32, 8, ROWS), axis=0)
        m_l = jnp.full((8, ROWS), NEG, jnp.float32)
        for j in range(8):
            t = jnp.max(s2[32 * j:32 * j + 32].reshape(4, 8, ROWS), axis=0)
            m_l = jnp.maximum(m_l, jnp.where(low_f[j], t, NEG))
            m_h = jnp.maximum(m_h, jnp.where(high_f[j], t, NEG))
        old_l, old_h = max_l[...], max_h[...]
        new_l = jnp.maximum(old_l, jnp.max(m_l, axis=0, keepdims=True))
        new_h = jnp.maximum(old_h, jnp.max(m_h, axis=0, keepdims=True))
        fade_l = jnp.exp2((old_l - new_l) * SCALE)
        fade_h = jnp.exp2((old_h - new_h) * SCALE)
        max_l[...] = new_l
        max_h[...] = new_h
        at_l = jnp.broadcast_to(new_l * SCALE, (8, ROWS))
        at_h = jnp.broadcast_to(new_h * SCALE, (8, ROWS))
        p1 = jnp.exp2(s1.reshape(32, 8, ROWS) * SCALE - at_h[None])
        t_h = sum_h[...] * fade_h + jnp.sum(p1, axis=0)
        t_l = sum_l[...] * fade_l
        p2 = []
        for j in range(8):
            m = jnp.where(low_f[j], at_l, jnp.where(high_f[j], at_h, -NEG))
            p = jnp.exp2(s2[32 * j:32 * j + 32].reshape(4, 8, ROWS) * SCALE - m[None])
            t = jnp.sum(p, axis=0)
            t_l = t_l + jnp.where(low_f[j], t, 0.0)
            t_h = t_h + jnp.where(high_f[j], t, 0.0)
            p2.append(p.reshape(32, ROWS))
        sum_l[...] = t_l
        sum_h[...] = t_h
        r1 = lax.dot_general(cat(vl), p1.reshape(256, ROWS).astype(jnp.bfloat16), TN,
                             preferred_element_type=jnp.float32)
        r2 = lax.dot_general(v2, cat(p2).astype(jnp.bfloat16), TN, preferred_element_type=jnp.float32)
        acc_l[...] = acc_l[...] * fade_l + r2[0:HEAD]
        acc_h[...] = acc_h[...] * fade_h + (r1 + r2[HEAD:2 * HEAD])

    for i in range(8):
        shared(0, zz(i) * 8, 8, i)
    for n, k in enumerate((0, -1, 1, 2)):
        shared(1, xx(k) * 16, 16, 8 + n)
    for n, k in enumerate((0, -1, 1, 2)):
        shared(2, y * 32 + xx(k) * 8, 8, 16 + n)
    for n, k in ((20, 0), (21, -1), (23, 1), (22, 2)):
        shared(2, (1 - y) * 32 + xx(k) * 8, 8, n)

    def rounds(r, carry):
        chunk(r // 8, r % 8)
        return carry

    lax.fori_loop(0, 24, rounds, 0)

    fin_l = acc_l[...] / jnp.sum(sum_l[...], axis=0, keepdims=True)
    fin_h = acc_h[...] / jnp.sum(sum_h[...], axis=0, keepdims=True)
    fin_a = jnp.where(own_first, fin_l, fin_h).T.astype(jnp.bfloat16)
    fin_b = jnp.where(own_first, fin_h, fin_l).T.astype(jnp.bfloat16)
    for h in range(HEADS):
        att[core, 0:RUN, h * HEAD:(h + 1) * HEAD] = fin_a[h * RUN:(h + 1) * RUN]
        att[core, RUN:TOK, h * HEAD:(h + 1) * HEAD] = fin_b[h * RUN:(h + 1) * RUN]
    att_copy = rcopy(att.at[core], att.at[core], att_sem.at[0], att_sem.at[1], partner)
    att_copy.start()
    w_own.wait()
    w_in.wait_recv()
    rcopy(att.at[1 - core], att.at[1 - core], att_sem.at[0], att_sem.at[1], partner).wait_recv()

    away = pl.multiple_of((1 - yh) * 96, 96)
    home = yh * 96
    first_hops, local_sends = [], []
    for j in range(NJ):
        w0 = wbuf[0:512, j * CW:(j + 1) * CW]
        w1 = wbuf[512:1024, j * CW:(j + 1) * CW]
        part = (jnp.dot(att[0], w0, preferred_element_type=jnp.float32)
                + jnp.dot(att[1], w1, preferred_element_type=jnp.float32))
        pbuf[j] = part.astype(jnp.bfloat16)
        sign = 1 if j % 2 == 0 else -1
        c = rcopy(pbuf.at[j, pl.ds(away, 96)], relay.at[j], rs_send.at[j], rs_recv.at[j], ring_y(sign, core))
        c.start()
        first_hops.append(c)
        c = rcopy(pbuf.at[j, pl.ds(pl.multiple_of(home + 48 * (1 - core), 48), 48)], lbuf.at[j],
                  lo_send.at[j], lo_recv.at[j], partner)
        c.start()
        local_sends.append(c)

    forwards = []
    for j in range(NJ):
        first_hops[j].wait_recv()
        sign = 1 if j % 2 == 0 else -1
        for e in range(2):
            c = rcopy(relay.at[j, pl.ds(48 * e, 48)], rbuf.at[core, j], fw_send.at[2 * j + e],
                      fw_recv.at[core, j], ring_y(sign, e))
            c.start()
            forwards.append(c)

    outs = []
    mine = pl.multiple_of(core * HALF, HALF)
    theirs = pl.multiple_of((1 - core) * HALF, HALF)
    for j in range(NJ):
        rcopy(rbuf.at[core, j], rbuf.at[core, j], fw_send.at[0], fw_recv.at[core, j], partner).wait_recv()
        own = pbuf[j, pl.ds(pl.multiple_of(home + 48 * core, 48), 48), :]
        obuf[core, j] = (own.astype(jnp.float32) + rbuf[core, j].astype(jnp.float32)).astype(jnp.bfloat16)
        c = pltpu.make_async_copy(obuf.at[core, j], out_ref.at[:, pl.ds(mine + j * CW, CW)], out_sem.at[2 * j])
        c.start()
        outs.append(c)
        local_sends[j].wait_recv()
        rcopy(rbuf.at[1 - core, j], rbuf.at[1 - core, j], fw_send.at[0], fw_recv.at[1 - core, j], partner).wait_recv()
        obuf[1 - core, j] = (lbuf[j].astype(jnp.float32) + rbuf[1 - core, j].astype(jnp.float32)).astype(jnp.bfloat16)
        c = pltpu.make_async_copy(obuf.at[1 - core, j], out_ref.at[:, pl.ds(theirs + j * CW, CW)], out_sem.at[2 * j + 1])
        c.start()
        outs.append(c)

    for c in sends + [w_far, att_copy] + first_hops + local_sends + forwards:
        c.wait_send()
    for c in outs:
        c.wait()


N_AG = 65
N_DD = 24


def shards(queries, keys, values, positions, out_weight):
    any_spec = pl.BlockSpec(memory_space=pl.ANY)
    dma = pltpu.SemaphoreType.DMA
    bf, f32 = jnp.bfloat16, jnp.float32
    return pl.pallas_call(
        kernel,
        out_shape=jax.ShapeDtypeStruct((48, NCOL), bf),
        in_specs=[any_spec] * 5,
        out_specs=any_spec,
        scratch_shapes=[
            pltpu.VMEM((3, 2, NCP, 4, 16, HEAD), bf),
            pltpu.VMEM((4, RUN, HEAD), bf),
            pltpu.VMEM((TOK, HEADS * HEAD), bf),
            pltpu.VMEM((2 * HEAD, ROWS), bf),
            pltpu.VMEM((HEAD, ROWS), f32),
            pltpu.VMEM((HEAD, ROWS), f32),
            pltpu.VMEM((8, ROWS), f32),
            pltpu.VMEM((8, ROWS), f32),
            pltpu.VMEM((1, ROWS), f32),
            pltpu.VMEM((1, ROWS), f32),
            pltpu.VMEM((2, TOK, 512), bf),
            pltpu.VMEM((1024, HALF), bf),
            pltpu.VMEM((NJ, TOK, CW), bf),
            pltpu.VMEM((NJ, 96, CW), bf),
            pltpu.VMEM((2, NJ, 48, CW), bf),
            pltpu.VMEM((NJ, 48, CW), bf),
            pltpu.VMEM((2, NJ, 48, CW), bf),
            pltpu.SMEM((NCP * TOK,), jnp.int32),
            dma((16,)),
            dma((2,)),
            dma((3,)),
            dma((N_AG,)),
            dma((N_AG,)),
            dma((N_DD,)),
            dma((N_DD,)),
            dma((2,)),
            dma((NJ,)),
            dma((NJ,)),
            dma((2 * NJ,)),
            dma((2, NJ)),
            dma((NJ,)),
            dma((NJ,)),
            dma((2 * NJ,)),
        ],
        compiler_params=pltpu.CompilerParams(collective_id=0, has_side_effects=True,
                                             vmem_limit_bytes=56 * 1024 * 1024),
    )(queries, keys, values, positions, out_weight)


def solution(mesh):
    in_specs = (P("cp", "tp"), P("cp", None), P("cp", None), P(), P("tp", None))
    out_specs = P(("cp", "tp"), None)
    return jax.shard_map(shards, mesh=mesh, in_specs=in_specs, out_specs=out_specs, check_vma=False)
```

```python
import functools
import math

import jax
import jax.numpy as jnp
from jax import lax
from jax.experimental import pallas as pl
from jax.experimental.pallas import tpu as pltpu
from jax.sharding import PartitionSpec as P

MESH = pl.DeviceIdType.MESH
HEAD = 128
GROUP = 8
NY, NX, NZ = 2, 4, 8
NCP = NY * NX * NZ
RUN = 96
TOK = 192
HEADS = 4
ROWS = RUN * HEADS
NCOL = 8192
HALF = NCOL // 2
NJ = 8
CW = HALF // NJ
SCALE = HEAD ** (-0.5) * math.log2(math.e)
NEG = -1e30


COPIES = (
    (0, 0, 0, 1, 2, 1), (3, 0, 0, 1, 2, 1), (6, -2, 0, 1, 1, 2), (6, 2, 0, 1, 1, -2), (6, -1, 0, 1, 1, 1),
    (6, 1, 0, 1, 1, -1), (1, 2, 0, 2, 0, 2), (1, -1, 0, 2, 0, 1), (1, 1, 0, 2, 0, -1), (4, -1, 0, 2, 1, 1),
    (4, 1, 0, 2, 1, -1), (5, -1, 0, 2, 0, 1), (5, 1, 0, 2, 0, -1), (6, -4, 0, 1, 1, 2), (6, -3, 0, 1, 1, 1),
    (6, 3, 0, 1, 1, -1), (4, -2, 0, 2, 1, 1), (5, 1, -1, 2, 0, -1), (5, -1, -1, 2, 0, 1), (4, 2, 0, 2, 1, -1),
    (5, 1, 1, 2, 0, -1), (5, -1, 1, 2, 0, 1), (2, -1, 0, 4, 1, 1), (2, 1, 1, 4, 1, -1), (2, 1, 0, 4, 1, -1),
    (2, -1, 1, 4, 1, 1), (5, 2, 0, 2, 0, 1), (7, -1, 0, 8, 0, 1), (7, 1, 0, 8, 0, -1), (8, 0, 0, 8, 2, 1),
    (4, -3, 0, 2, 1, 1), (5, -1, -2, 2, 0, 1), (5, 1, -2, 2, 0, -1), (5, 2, -1, 2, 0, -1), (4, 3, 0, 2, 1, -1),
    (5, -1, 2, 2, 0, 1), (5, 1, 2, 2, 0, -1), (5, 2, 1, 2, 0, -1), (2, -2, 0, 4, 1, 1), (2, 2, 1, 4, 1, -1),
    (2, -2, 1, 4, 1, 1), (2, 2, 0, 4, 1, -1), (7, 2, 1, 4, 0, -1), (8, 1, 0, 8, 2, 1), (4, -4, 0, 2, 1, 1),
    (5, 1, -3, 2, 0, -1), (5, -1, -3, 2, 0, 1), (5, 1, 3, 2, 0, -1), (5, -1, 3, 2, 0, 1), (7, 2, 0, 4, 0, 1),
    (8, -1, 0, 8, 2, 1), (5, 2, -2, 2, 0, 1), (5, 2, 2, 2, 0, 1), (2, -3, 0, 4, 1, 1), (2, 3, 1, 4, 1, -1),
    (2, -3, 1, 4, 1, 1), (2, 3, 0, 4, 1, -1), (5, -1, -4, 2, 0, 1), (5, 1, -4, 2, 0, -1), (5, 2, -3, 2, 0, -1),
    (5, 2, 3, 2, 0, -1), (8, 2, 0, 8, 2, 1), (2, -4, 0, 4, 1, 1), (2, 4, 1, 4, 1, -1), (5, 2, -4, 2, 0, 1),
)
GROUPS = (
    (0, 0, 0), (2, 0, 0), (0, -1, 0), (0, 1, 0), (2, 1, 0), (2, 0, 1), (2, -1, 0), (0, -2, 0), (0, 2, 0), (1, 0, 0),
    (2, 1, 1), (2, 2, 0), (1, -1, 0), (1, 1, 0), (2, -1, 1), (0, -3, 0), (0, 3, 0), (1, 2, 0), (0, -4, 0),
    (2, 2, 1),
)
FIRST = 6
ROUNDS = (
    (0, 0, (0, 106, 107, 108, 1, 109, 110, 111, 112, 4, 5, 2, 113, 114, 3, 115, 8, 9, 116, 117, 118, 10, 119, 120, 121, 12, 15, 7, 6, 122, 123, 124, 125, 200, 14, 11, 126, 13, 127, 128, 129, 201)),
    (1, 0, ()),
    (2, 0, (16, 130, 131, 132, 17, 133, 18, 19, 134, 135, 136, 20, 137, 21, 26, 22, 138, 23, 139, 25, 140, 202, 24, 141, 203, 28, 142, 143, 204, 29, 205, 30, 144, 145, 146, 34, 147, 148, 27, 149, 150, 206, 32)),
    (3, 0, (31, 151, 33)), (4, 0, (35, 152, 36)), (5, 0, (38, 153, 39, 154, 37)), (6, 0, ()),
    (7, 0, (40, 155, 207, 41, 156, 208, 46, 42, 44, 157, 158, 209, 48, 45, 159)),
    (8, 0, (47, 160, 43, 210, 49, 161, 211)), (9, 0, (51,)), (9, 1, (53, 162, 54, 163, 52)),
    (10, 0, (57, 164, 212, 58, 213)), (11, 0, (50, 214, 55, 215, 56, 216, 59)), (12, 0, (60,)), (12, 1, ()),
    (13, 0, ()), (13, 1, ()), (14, 0, (62, 64, 217, 63, 218, 61, 219)), (15, 0, ()), (16, 0, ()), (17, 0, ()),
    (17, 1, ()), (18, 0, ()), (19, 0, ()),
)


def place(copy, x, z, y):
    kind, k0, k1, n = copy[:4]
    at_x, at_z, at_y = (x + k0 + NX) % NX, (z + k0 + NZ) % NZ, 1 - y
    slot = (
        z * 8 + x * 2 + at_y,
        z * 8 + at_x * 2,
        at_z * 8 + k1 * 4,
        x * 16 + z * 2 + at_y,
        x * 16 + at_z * 2,
        at_x * 16 + (z + k1 + NZ) % NZ * 2,
        y * 32 + x * 8 + at_z,
        y * 32 + at_x * 8 + k1 * 4,
        at_y * 32 + at_x * 8,
    )[kind]
    return kind // 3, slot, n


def group_place(group, x, z, y):
    f, k0, k1 = group
    at_x = (x + k0 + NX) % NX
    slot = ((z + k0 + NZ) % NZ * 8, at_x * 16, (y + k1) % 2 * 32 + at_x * 8)[f]
    return f, slot, 16 if f == 1 else 8


def chunk_code(group, half):
    f, k0, k1 = group
    return f * 64 + k0 % 8 * 4 + (k1 if f == 2 else half)


def kernel(q_ref, k_ref, v_ref, pos_ref, w_ref, out_ref,
           kv, own_kv, qv, q2t, acc_l, acc_h, sum_l, sum_h, max_l, max_h,
           s1, s2, p1, p2, vl, v2, top_l, top_h, fade_l, fade_h,
           att, wbuf, pbuf, rbuf, lbuf, obuf, pos, flags,
           fill_sem, in_sem, w_sem, ag_send, ag_recv, dd_send, dd_recv,
           att_sem, rs_send, rs_recv, lo_send, lo_recv, out_sem):
    cp = lax.axis_index("cp")
    tp = lax.axis_index("tp")
    core = tp % 2
    yh = tp // 2
    z = cp % NZ
    x = (cp // NZ) % NX
    y = cp // (NZ * NX)

    def cp_of(yy, xx, zz):
        return (yy * NX + xx) * NZ + zz

    partner = dict(cp=cp, tp=yh * 2 + 1 - core)

    def zz(k):
        return (z + k + NZ) % NZ

    def xx(k):
        return (x + k + NX) % NX

    def at_z(k):
        return dict(cp=cp_of(y, x, zz(k)), tp=tp)

    def at_x(k):
        return dict(cp=cp_of(y, xx(k), z), tp=tp)

    flip = dict(cp=cp_of(1 - y, x, z), tp=tp)
    away_cores = [dict(cp=cp, tp=(1 - yh) * 2 + e) for e in (0, 1)]

    q_copy = pltpu.make_async_copy(q_ref, qv, in_sem.at[0])
    q_copy.start()
    pos_copy = pltpu.make_async_copy(pos_ref, pos, in_sem.at[1])
    pos_copy.start()
    slot_a = z * 8 + x * 2 + y
    slot_b = x * 16 + z * 2 + y
    slot_d = y * 32 + x * 8 + z
    own_slots = (slot_a, slot_b, slot_d)
    fills = []
    cols = pl.ds(pl.multiple_of(yh * HEAD, HEAD), HEAD)
    for f in range(3):
        for h in range(2):
            for src, kind in ((k_ref, 0), (v_ref, 2)):
                rows = pl.ds(pl.multiple_of(h * RUN + 32 * f + 16 * core, 16), 16)
                fills.append(pltpu.make_async_copy(
                    src.at[rows, cols], kv.at[f, core, own_slots[f], kind + h], fill_sem.at[len(fills)]))
    own_fills = []
    for h in range(2):
        for src, kind in ((k_ref, 0), (v_ref, 2)):
            own_fills.append(pltpu.make_async_copy(
                src.at[pl.ds(h * RUN, RUN), cols], own_kv.at[kind + h], fill_sem.at[12 + len(own_fills)]))
    for c in fills + own_fills:
        c.start()

    barrier = pltpu.get_barrier_semaphore()
    peers = [at_z(k) for k in (1, -1, 2, -2)] + [at_x(k) for k in (1, -1, 2)] + [partner, flip] + away_cores
    for p in peers:
        pl.semaphore_signal(barrier, inc=1, device_id=p, device_id_type=MESH)
    pl.semaphore_wait(barrier, len(peers))
    for c in fills:
        c.wait()

    def rcopy(src, dst, ssem, rsem, dev):
        return pltpu.make_async_remote_copy(src_ref=src, dst_ref=dst, send_sem=ssem, recv_sem=rsem,
                                            device_id=dev, device_id_type=MESH)

    def part(owner, where):
        f, slot, n = where
        return kv.at[f, owner, pl.ds(slot, n)]

    def gather(i):
        axis, steps = COPIES[i][4:]
        dev = (at_x, at_z, lambda k: flip)[axis](steps)
        where = place(COPIES[i], xx(steps) if axis == 0 else x, zz(steps) if axis == 1 else z, 1 - y if axis == 2 else y)
        ref = part(core, where)
        return rcopy(ref, ref, ag_send.at[i], ag_recv.at[i], dev)

    def arrive(i):
        ref = part(core, place(COPIES[i], x, z, y))
        return rcopy(ref, ref, ag_send.at[i], ag_recv.at[i], partner)

    def share(i, owner):
        ref = part(owner, group_place(GROUPS[i], x, z, y))
        return rcopy(ref, ref, dd_send.at[i], dd_recv.at[i], partner)

    for i in range(FIRST):
        gather(i).start()

    my_rows = pl.ds(pl.multiple_of(core * 512, 512), 512)
    w_own = pltpu.make_async_copy(
        w_ref.at[:, pl.ds(pl.multiple_of(core * HALF, HALF), HALF)], wbuf.at[my_rows], w_sem.at[0])
    w_own.start()
    w_far = rcopy(w_ref.at[:, pl.ds(pl.multiple_of((1 - core) * HALF, HALF), HALF)], wbuf.at[my_rows],
                  w_sem.at[1], w_sem.at[2], partner)
    w_far.start()
    other_rows = pl.ds(pl.multiple_of((1 - core) * 512, 512), 512)
    w_in = rcopy(w_ref.at[:, pl.ds(0, HALF)], wbuf.at[other_rows], w_sem.at[1], w_sem.at[2], partner)

    q_copy.wait()
    pos_copy.wait()
    own0 = pos[cp * TOK]
    own1 = pos[cp * TOK + RUN]
    own_first = own0 < own1
    own_low = jnp.minimum(own0, own1)

    qa = jnp.concatenate([qv[0:RUN, h * HEAD:(h + 1) * HEAD] for h in range(HEADS)], axis=0)
    qb = jnp.concatenate([qv[RUN:TOK, h * HEAD:(h + 1) * HEAD] for h in range(HEADS)], axis=0)
    q2t[0:HEAD, :] = jnp.where(own_first, qa, qb).T
    q2t[HEAD:2 * HEAD, :] = jnp.where(own_first, qb, qa).T

    TN = (((0,), (0,)), ((), ()))

    for c in own_fills:
        c.wait()

    lane = lax.broadcasted_iota(jnp.int32, (RUN, ROWS), 1)
    keep = lax.broadcasted_iota(jnp.int32, (RUN, ROWS), 0) <= lane % RUN

    def triangle(kk, vv, qt, acc, total, top):
        s = jnp.dot(kk, qt, preferred_element_type=jnp.float32)
        s = jnp.where(keep, s, NEG)
        m = jnp.max(s, axis=0, keepdims=True)
        p = jnp.exp2(s * SCALE - m * SCALE)
        top[...] = m
        total[...] = jnp.sum(p.reshape(RUN // 8, 8, ROWS), axis=0)
        acc[...] = lax.dot_general(vv, p.astype(jnp.bfloat16), TN, preferred_element_type=jnp.float32)

    k0, k1, v0, v1 = (own_kv[i] for i in range(4))
    triangle(jnp.where(own_first, k0, k1), jnp.where(own_first, v0, v1), q2t[0:HEAD, :], acc_l, sum_l, max_l)
    triangle(jnp.where(own_first, k1, k0), jnp.where(own_first, v1, v0), q2t[HEAD:2 * HEAD, :], acc_h, sum_h, max_h)

    zero = jnp.zeros((16, HEAD), jnp.bfloat16)

    cat = functools.partial(jnp.concatenate, axis=0)

    def scores(f, i, r):
        kl, vl_, ka, kb, va, vb, low_f, high_f = ([] for _ in range(8))
        for j in range(8):
            s_z = jnp.where(f == 0, i, jnp.where(f == 1, (i % 2) * 4 + j // 2, j))
            s_x = jnp.where(f == 0, j // 2, jnp.where(f == 1, i // 2, i % 4))
            s_y = jnp.where(f == 2, i // 4, j % 2)
            s = cp_of(s_y, s_x, s_z)
            r0 = pos[s * TOK]
            r1 = pos[s * TOK + RUN]
            first = r0 < r1
            low = jnp.minimum(r0, r1) < own_low
            high = jnp.minimum(r0, r1) > own_low
            low_f.append(low)
            high_f.append(high)
            flags[j] = jnp.where(low, 1, 0)
            flags[8 + j] = jnp.where(high, 1, 0)
            for c in range(2):
                t0, t1, u0, u1 = (kv[f, c, i * 8 + j, n] for n in range(4))
                kl.append(jnp.where(first, t0, t1))
                vl_.append(jnp.where(first, u0, u1))
                ka.append(jnp.where(low, kl[-1], zero))
                va.append(jnp.where(low, vl_[-1], zero))
                kb.append(jnp.where(high, jnp.where(first, t1, t0), zero))
                vb.append(jnp.where(high, jnp.where(first, u1, u0), zero))
        vl[r % 2] = cat(vl_)
        v2[r % 2, :, 0:HEAD] = cat(va)
        v2[r % 2, :, HEAD:2 * HEAD] = cat(vb)
        k2 = jnp.concatenate([cat(ka), cat(kb)], axis=1)
        a = jnp.dot(cat(kl), q2t[HEAD:2 * HEAD, :], preferred_element_type=jnp.float32)
        b = jnp.dot(k2, q2t[...], preferred_element_type=jnp.float32)
        s1[...] = a
        s2[...] = b
        m_h = jnp.max(a.reshape(32, 8, ROWS), axis=0)
        m_l = jnp.full((8, ROWS), NEG, jnp.float32)
        for j in range(8):
            t = jnp.max(b[32 * j:32 * j + 32].reshape(4, 8, ROWS), axis=0)
            m_l = jnp.maximum(m_l, jnp.where(low_f[j], t, NEG))
            m_h = jnp.maximum(m_h, jnp.where(high_f[j], t, NEG))
        top_l[...] = m_l
        top_h[...] = m_h

    def weigh():
        old_l, old_h = max_l[...], max_h[...]
        new_l = jnp.maximum(old_l, jnp.max(top_l[...], axis=0, keepdims=True))
        new_h = jnp.maximum(old_h, jnp.max(top_h[...], axis=0, keepdims=True))
        f_l = jnp.exp2((old_l - new_l) * SCALE)
        f_h = jnp.exp2((old_h - new_h) * SCALE)
        max_l[...] = new_l
        max_h[...] = new_h
        fade_l[...] = f_l
        fade_h[...] = f_h
        at_l = jnp.broadcast_to(new_l * SCALE, (8, ROWS))
        at_h = jnp.broadcast_to(new_h * SCALE, (8, ROWS))
        t_h = sum_h[...] * f_h
        t_l = sum_l[...] * f_l
        for j in range(8):
            rows = slice(32 * j, 32 * j + 32)
            p = jnp.exp2(s1[rows, :].reshape(4, 8, ROWS) * SCALE - at_h[None])
            t_h = t_h + jnp.sum(p, axis=0)
            p1[rows, :] = p.reshape(32, ROWS).astype(jnp.bfloat16)
            low, high = flags[j] > 0, flags[8 + j] > 0
            m = jnp.where(low, at_l, jnp.where(high, at_h, -NEG))
            p = jnp.exp2(s2[rows, :].reshape(4, 8, ROWS) * SCALE - m[None])
            t = jnp.sum(p, axis=0)
            t_l = t_l + jnp.where(low, t, 0.0)
            t_h = t_h + jnp.where(high, t, 0.0)
            p2[rows, :] = p.reshape(32, ROWS).astype(jnp.bfloat16)
        sum_l[...] = t_l
        sum_h[...] = t_h

    def attend(r):
        r1 = lax.dot_general(vl[r % 2], p1[...], TN, preferred_element_type=jnp.float32)
        r2 = lax.dot_general(v2[r % 2], p2[...], TN, preferred_element_type=jnp.float32)
        acc_l[...] = acc_l[...] * fade_l[...] + r2[0:HEAD]
        acc_h[...] = acc_h[...] * fade_h[...] + (r1 + r2[HEAD:2 * HEAD])

    for ref in (s1, s2, top_l, top_h):
        ref[...] = jnp.full(ref.shape, NEG, jnp.float32)
    for ref in (p1, p2, vl, v2):
        ref[...] = jnp.zeros(ref.shape, jnp.bfloat16)
    fade_l[...] = jnp.ones((1, ROWS), jnp.float32)
    fade_h[...] = jnp.ones((1, ROWS), jnp.float32)
    for j in range(16):
        flags[j] = jnp.int32(1)

    met = set()
    codes = [chunk_code(GROUPS[g], half) for g, half, _ in ROUNDS]

    def rounds(r, carry):
        for i, (g, half, events) in enumerate(ROUNDS):
            if not events and g in met:
                continue

            @pl.when(r == i)
            def _():
                for e in events:
                    if e < 100:
                        arrive(e).wait_recv()
                    elif e < 200:
                        gather(e - 100).start()
                    else:
                        share(e - 200, core).start()
                if g not in met:
                    share(g, 1 - core).wait_recv()

            met.add(g)
        code = jnp.int32(0)
        for i, c in enumerate(codes):
            code = jnp.where(r == i, c, code)
        f, k0, k1 = code // 64, code // 4 % 8, code % 4
        i = jnp.where(f == 0, (z + k0) % NZ,
                      jnp.where(f == 1, (x + k0) % NX * 2 + k1, (y + k1) % 2 * 4 + (x + k0) % NX))
        attend(r)
        weigh()
        scores(f, i, r)
        return carry

    lax.fori_loop(0, len(ROUNDS), rounds, 0)
    attend(len(ROUNDS))
    weigh()
    attend(len(ROUNDS) + 1)

    fin_l = acc_l[...] / jnp.sum(sum_l[...], axis=0, keepdims=True)
    fin_h = acc_h[...] / jnp.sum(sum_h[...], axis=0, keepdims=True)
    fin_a = jnp.where(own_first, fin_l, fin_h).T.astype(jnp.bfloat16)
    fin_b = jnp.where(own_first, fin_h, fin_l).T.astype(jnp.bfloat16)
    for h in range(HEADS):
        att[core, 0:RUN, h * HEAD:(h + 1) * HEAD] = fin_a[h * RUN:(h + 1) * RUN]
        att[core, RUN:TOK, h * HEAD:(h + 1) * HEAD] = fin_b[h * RUN:(h + 1) * RUN]
    att_copy = rcopy(att.at[core], att.at[core], att_sem.at[0], att_sem.at[1], partner)
    att_copy.start()
    w_own.wait()
    w_in.wait_recv()
    rcopy(att.at[1 - core], att.at[1 - core], att_sem.at[0], att_sem.at[1], partner).wait_recv()

    home = yh * 96
    far_sends, local_sends = [], []
    for j in range(NJ):
        w0 = wbuf[0:512, j * CW:(j + 1) * CW]
        w1 = wbuf[512:1024, j * CW:(j + 1) * CW]
        product = (jnp.dot(att[0], w0, preferred_element_type=jnp.float32)
                   + jnp.dot(att[1], w1, preferred_element_type=jnp.float32))
        pbuf[j] = product.astype(jnp.bfloat16)
        for e in range(2):
            rows = pl.ds(pl.multiple_of((1 - yh) * 96 + 48 * e, 48), 48)
            c = rcopy(pbuf.at[j, rows], rbuf.at[core, j], rs_send.at[2 * j + e], rs_recv.at[core, j], away_cores[e])
            c.start()
            far_sends.append(c)
        c = rcopy(pbuf.at[j, pl.ds(pl.multiple_of(home + 48 * (1 - core), 48), 48)], lbuf.at[j],
                  lo_send.at[j], lo_recv.at[j], partner)
        c.start()
        local_sends.append(c)

    outs = []
    mine = pl.multiple_of(core * HALF, HALF)
    theirs = pl.multiple_of((1 - core) * HALF, HALF)
    for j in range(NJ):
        rcopy(rbuf.at[core, j], rbuf.at[core, j], rs_send.at[0], rs_recv.at[core, j], partner).wait_recv()
        own = pbuf[j, pl.ds(pl.multiple_of(home + 48 * core, 48), 48), :]
        obuf[core, j] = (own.astype(jnp.float32) + rbuf[core, j].astype(jnp.float32)).astype(jnp.bfloat16)
        c = pltpu.make_async_copy(obuf.at[core, j], out_ref.at[:, pl.ds(mine + j * CW, CW)], out_sem.at[2 * j])
        c.start()
        outs.append(c)
        local_sends[j].wait_recv()
        rcopy(rbuf.at[1 - core, j], rbuf.at[1 - core, j], rs_send.at[0], rs_recv.at[1 - core, j], partner).wait_recv()
        obuf[1 - core, j] = (lbuf[j].astype(jnp.float32) + rbuf[1 - core, j].astype(jnp.float32)).astype(jnp.bfloat16)
        c = pltpu.make_async_copy(obuf.at[1 - core, j], out_ref.at[:, pl.ds(theirs + j * CW, CW)], out_sem.at[2 * j + 1])
        c.start()
        outs.append(c)

    sends = [gather(i) for i in range(len(COPIES))] + [share(i, core) for i in range(len(GROUPS))]
    for c in sends + [w_far, att_copy] + far_sends + local_sends:
        c.wait_send()
    for c in outs:
        c.wait()


def shards(queries, keys, values, positions, out_weight):
    any_spec = pl.BlockSpec(memory_space=pl.ANY)
    dma = pltpu.SemaphoreType.DMA
    bf, f32 = jnp.bfloat16, jnp.float32
    return pl.pallas_call(
        kernel,
        out_shape=jax.ShapeDtypeStruct((48, NCOL), bf),
        in_specs=[any_spec] * 5,
        out_specs=any_spec,
        scratch_shapes=[
            pltpu.VMEM((3, 2, NCP, 4, 16, HEAD), bf),
            pltpu.VMEM((4, RUN, HEAD), bf),
            pltpu.VMEM((TOK, HEADS * HEAD), bf),
            pltpu.VMEM((2 * HEAD, ROWS), bf),
            pltpu.VMEM((HEAD, ROWS), f32),
            pltpu.VMEM((HEAD, ROWS), f32),
            pltpu.VMEM((8, ROWS), f32),
            pltpu.VMEM((8, ROWS), f32),
            pltpu.VMEM((1, ROWS), f32),
            pltpu.VMEM((1, ROWS), f32),
            pltpu.VMEM((256, ROWS), f32),
            pltpu.VMEM((256, ROWS), f32),
            pltpu.VMEM((256, ROWS), bf),
            pltpu.VMEM((256, ROWS), bf),
            pltpu.VMEM((2, 256, HEAD), bf),
            pltpu.VMEM((2, 256, 2 * HEAD), bf),
            pltpu.VMEM((8, ROWS), f32),
            pltpu.VMEM((8, ROWS), f32),
            pltpu.VMEM((1, ROWS), f32),
            pltpu.VMEM((1, ROWS), f32),
            pltpu.VMEM((2, TOK, 512), bf),
            pltpu.VMEM((1024, HALF), bf),
            pltpu.VMEM((NJ, TOK, CW), bf),
            pltpu.VMEM((2, NJ, 48, CW), bf),
            pltpu.VMEM((NJ, 48, CW), bf),
            pltpu.VMEM((2, NJ, 48, CW), bf),
            pltpu.SMEM((NCP * TOK,), jnp.int32),
            pltpu.SMEM((16,), jnp.int32),
            dma((16,)),
            dma((2,)),
            dma((3,)),
            dma((len(COPIES),)),
            dma((len(COPIES),)),
            dma((len(GROUPS),)),
            dma((len(GROUPS),)),
            dma((2,)),
            dma((2 * NJ,)),
            dma((2, NJ)),
            dma((NJ,)),
            dma((NJ,)),
            dma((2 * NJ,)),
        ],
        compiler_params=pltpu.CompilerParams(collective_id=0, has_side_effects=True,
                                             vmem_limit_bytes=56 * 1024 * 1024),
    )(queries, keys, values, positions, out_weight)


def solution(mesh):
    in_specs = (P("cp", "tp"), P("cp", None), P("cp", None), P(), P("tp", None))
    out_specs = P(("cp", "tp"), None)
    return jax.shard_map(shards, mesh=mesh, in_specs=in_specs, out_specs=out_specs, check_vma=False)
```

```python
import functools
import math

import jax
import jax.numpy as jnp
from jax import lax
from jax.experimental import pallas as pl
from jax.experimental.pallas import tpu as pltpu
from jax.sharding import PartitionSpec as P

MESH = pl.DeviceIdType.MESH
HEAD = 128
GROUP = 8
NY, NX, NZ = 2, 4, 8
NCP = NY * NX * NZ
RUN = 96
TOK = 192
HEADS = 4
ROWS = RUN * HEADS
NCOL = 8192
HALF = NCOL // 2
NJ = 8
CW = HALF // NJ
SCALE = HEAD ** (-0.5) * math.log2(math.e)
NEG = -1e30


COPIES = (
    (0, 0, 0, 1, 2, 1), (6, -2, 0, 1, 1, 2), (6, 2, 0, 1, 1, -2), (3, 0, 0, 1, 2, 1), (6, -1, 0, 1, 1, 1),
    (6, 1, 0, 1, 1, -1), (1, 2, 0, 2, 0, 2), (1, -1, 0, 2, 0, 1), (1, 1, 0, 2, 0, -1), (4, -2, 0, 2, 1, 2),
    (4, 2, 0, 2, 1, -2), (4, -1, 0, 2, 1, 1), (4, 1, 0, 2, 1, -1), (5, -1, 0, 2, 0, 1), (5, 1, 0, 2, 0, -1),
    (6, -4, 0, 1, 1, 2), (6, -3, 0, 1, 1, 1), (6, 3, 0, 1, 1, -1), (2, -1, 0, 4, 1, 1), (2, 1, 1, 4, 1, -1),
    (2, 1, 0, 4, 1, -1), (2, -1, 1, 4, 1, 1), (5, 1, -1, 2, 0, -1), (5, -1, -1, 2, 0, 1), (5, 1, 1, 2, 0, -1),
    (5, -1, 1, 2, 0, 1), (4, -4, 0, 2, 1, 2), (4, -3, 0, 2, 1, 1), (5, -1, -2, 2, 0, 1), (5, 1, -2, 2, 0, -1),
    (4, 3, 0, 2, 1, -1), (5, -1, 2, 2, 0, 1), (5, 1, 2, 2, 0, -1), (5, 2, 0, 2, 0, 1), (7, -1, 0, 8, 0, 1),
    (7, 1, 0, 8, 0, -1), (8, 0, 0, 8, 2, 1), (5, 2, -1, 2, 0, -1), (2, -2, 0, 4, 1, 1), (2, 2, 1, 4, 1, -1),
    (5, 2, 1, 2, 0, -1), (5, 2, -2, 2, 0, 1), (2, -2, 1, 4, 1, 1), (2, 2, 0, 4, 1, -1), (5, 2, 2, 2, 0, 1),
    (5, 1, 3, 2, 0, -1), (5, -1, 3, 2, 0, 1), (5, 1, -3, 2, 0, -1), (5, -1, -3, 2, 0, 1), (5, -1, -4, 2, 0, 1),
    (5, 1, -4, 2, 0, -1), (7, 2, 1, 4, 0, -1), (8, 1, 0, 8, 2, 1), (7, 2, 0, 4, 0, 1), (8, -1, 0, 8, 2, 1),
    (2, -3, 0, 4, 1, 1), (2, 3, 1, 4, 1, -1), (2, -3, 1, 4, 1, 1), (5, 2, 3, 2, 0, -1), (2, 3, 0, 4, 1, -1),
    (5, 2, -3, 2, 0, -1), (5, 2, -4, 2, 0, 1), (8, 2, 0, 8, 2, 1), (2, -4, 0, 4, 1, 1), (2, 4, 1, 4, 1, -1),
)
GROUPS = (
    (0, 0, 0), (2, 0, 0), (0, -1, 0), (0, 1, 0), (2, 0, 1), (1, 0, 0), (2, 1, 0), (2, -1, 0), (0, -2, 0), (0, 2, 0),
    (1, 1, 0), (1, -1, 0), (2, 2, 0), (2, 1, 1), (0, -3, 0), (0, 3, 0), (1, 2, 0), (2, -1, 1), (0, -4, 0),
    (2, 2, 1),
)
FIRST = 6
ROUNDS = (
    (0, 0, (0, 106, 107, 108, 3, 109, 110, 111, 112, 113, 114, 4, 5, 1, 115, 116, 2, 117, 8, 14, 7, 6, 118, 119, 120, 121, 200, 11, 122, 123, 12, 124, 125, 9, 126, 127, 128, 129, 10, 130, 131, 132, 13, 133, 17, 16, 15, 134, 135, 136, 201)),
    (1, 0, ()),
    (2, 0, (22, 137, 23, 18, 138, 19, 139, 24, 140, 25, 29, 28, 141, 21, 142, 202, 20, 143, 203, 32, 31, 144, 30, 145, 146, 33)),
    (3, 0, (36, 204, 27, 147, 148, 26, 149, 150, 205)),
    (4, 0, (35, 151, 152, 206, 37, 34, 153, 154, 207, 38, 155, 39, 156)), (5, 0, (40, 41)),
    (5, 1, (44, 42, 157, 208, 45, 158, 43, 159, 209, 46)), (6, 0, ()), (7, 0, (47, 160, 48)),
    (8, 0, (50, 210, 49, 161, 211)), (9, 0, ()), (10, 0, (51, 53, 162, 212, 55, 163, 56, 164)),
    (10, 1, (52, 213, 58)), (11, 0, (57, 214, 59, 215)), (11, 1, (60,)), (12, 0, (61, 216)), (13, 0, (54, 217)),
    (14, 0, ()), (15, 0, ()), (16, 0, (63, 64, 218)), (16, 1, ()), (17, 0, (62, 219)), (18, 0, ()), (19, 0, ()),
)


def place(copy, x, z, y):
    kind, k0, k1, n = copy[:4]
    at_x, at_z, at_y = (x + k0 + NX) % NX, (z + k0 + NZ) % NZ, 1 - y
    slot = (
        z * 8 + x * 2 + at_y,
        z * 8 + at_x * 2,
        at_z * 8 + k1 * 4,
        x * 16 + z * 2 + at_y,
        x * 16 + at_z * 2,
        at_x * 16 + (z + k1 + NZ) % NZ * 2,
        y * 32 + x * 8 + at_z,
        y * 32 + at_x * 8 + k1 * 4,
        at_y * 32 + at_x * 8,
    )[kind]
    return kind // 3, slot, n


def group_place(group, x, z, y):
    f, k0, k1 = group
    at_x = (x + k0 + NX) % NX
    slot = ((z + k0 + NZ) % NZ * 8, at_x * 16, (y + k1) % 2 * 32 + at_x * 8)[f]
    return f, slot, 16 if f == 1 else 8


def chunk_code(group, half):
    f, k0, k1 = group
    return f * 64 + k0 % 8 * 4 + (k1 if f == 2 else half)


def kernel(q_ref, k_ref, v_ref, pos_ref, w_ref, out_ref,
           kv, own_kv, qv, q2t, acc_l, acc_h, sum_l, sum_h, max_l, max_h,
           s1, s2, p1, p2, vl, v2, top_l, top_h, fade_l, fade_h,
           att, wbuf, pbuf, rbuf, lbuf, pos, flags,
           fill_sem, in_sem, w_sem, ag_send, ag_recv, dd_send, dd_recv,
           att_sem, rs_send, rs_recv, lo_send, lo_recv):
    cp = lax.axis_index("cp")
    tp = lax.axis_index("tp")
    core = tp % 2
    yh = tp // 2
    z = cp % NZ
    x = (cp // NZ) % NX
    y = cp // (NZ * NX)

    def cp_of(yy, xx, zz):
        return (yy * NX + xx) * NZ + zz

    partner = dict(cp=cp, tp=yh * 2 + 1 - core)

    def zz(k):
        return (z + k + NZ) % NZ

    def xx(k):
        return (x + k + NX) % NX

    def at_z(k):
        return dict(cp=cp_of(y, x, zz(k)), tp=tp)

    def at_x(k):
        return dict(cp=cp_of(y, xx(k), z), tp=tp)

    flip = dict(cp=cp_of(1 - y, x, z), tp=tp)
    away_cores = [dict(cp=cp, tp=(1 - yh) * 2 + e) for e in (0, 1)]

    q_copy = pltpu.make_async_copy(q_ref, qv, in_sem.at[0])
    q_copy.start()
    pos_copy = pltpu.make_async_copy(pos_ref, pos, in_sem.at[1])
    pos_copy.start()
    slot_a = z * 8 + x * 2 + y
    slot_b = x * 16 + z * 2 + y
    slot_d = y * 32 + x * 8 + z
    own_slots = (slot_a, slot_b, slot_d)
    fills = []
    cols = pl.ds(pl.multiple_of(yh * HEAD, HEAD), HEAD)
    for f in range(3):
        for h in range(2):
            for src, kind in ((k_ref, 0), (v_ref, 2)):
                rows = pl.ds(pl.multiple_of(h * RUN + 32 * f + 16 * core, 16), 16)
                fills.append(pltpu.make_async_copy(
                    src.at[rows, cols], kv.at[f, core, own_slots[f], kind + h], fill_sem.at[len(fills)]))
    own_fills = []
    for h in range(2):
        for src, kind in ((k_ref, 0), (v_ref, 2)):
            own_fills.append(pltpu.make_async_copy(
                src.at[pl.ds(h * RUN, RUN), cols], own_kv.at[kind + h], fill_sem.at[12 + len(own_fills)]))
    for c in fills + own_fills:
        c.start()

    barrier = pltpu.get_barrier_semaphore()
    x_steps = sorted({sign * c[5] % NX for c in COPIES if c[4] == 0 for sign in (1, -1)})
    z_steps = sorted({sign * c[5] % NZ for c in COPIES if c[4] == 1 for sign in (1, -1)})
    peers = [at_z(k) for k in z_steps] + [at_x(k) for k in x_steps] + [partner, flip] + away_cores
    for p in peers:
        pl.semaphore_signal(barrier, inc=1, device_id=p, device_id_type=MESH)
    pl.semaphore_wait(barrier, len(peers))
    for c in fills:
        c.wait()

    def rcopy(src, dst, ssem, rsem, dev):
        return pltpu.make_async_remote_copy(src_ref=src, dst_ref=dst, send_sem=ssem, recv_sem=rsem,
                                            device_id=dev, device_id_type=MESH)

    def part(owner, where):
        f, slot, n = where
        return kv.at[f, owner, pl.ds(slot, n)]

    def gather(i):
        axis, steps = COPIES[i][4:]
        dev = (at_x, at_z, lambda k: flip)[axis](steps)
        where = place(COPIES[i], xx(steps) if axis == 0 else x, zz(steps) if axis == 1 else z, 1 - y if axis == 2 else y)
        ref = part(core, where)
        return rcopy(ref, ref, ag_send.at[i], ag_recv.at[i], dev)

    def arrive(i):
        ref = part(core, place(COPIES[i], x, z, y))
        return rcopy(ref, ref, ag_send.at[i], ag_recv.at[i], partner)

    def share(i, owner):
        ref = part(owner, group_place(GROUPS[i], x, z, y))
        return rcopy(ref, ref, dd_send.at[i], dd_recv.at[i], partner)

    for i in range(FIRST):
        gather(i).start()

    my_rows = pl.ds(pl.multiple_of(core * 512, 512), 512)
    w_own = pltpu.make_async_copy(
        w_ref.at[:, pl.ds(pl.multiple_of(core * HALF, HALF), HALF)], wbuf.at[my_rows], w_sem.at[0])
    w_own.start()
    w_far = rcopy(w_ref.at[:, pl.ds(pl.multiple_of((1 - core) * HALF, HALF), HALF)], wbuf.at[my_rows],
                  w_sem.at[1], w_sem.at[2], partner)
    w_far.start()
    other_rows = pl.ds(pl.multiple_of((1 - core) * 512, 512), 512)
    w_in = rcopy(w_ref.at[:, pl.ds(0, HALF)], wbuf.at[other_rows], w_sem.at[1], w_sem.at[2], partner)

    q_copy.wait()
    pos_copy.wait()
    own0 = pos[cp * TOK]
    own1 = pos[cp * TOK + RUN]
    own_first = own0 < own1
    own_low = jnp.minimum(own0, own1)

    qa = jnp.concatenate([qv[0:RUN, h * HEAD:(h + 1) * HEAD] for h in range(HEADS)], axis=0)
    qb = jnp.concatenate([qv[RUN:TOK, h * HEAD:(h + 1) * HEAD] for h in range(HEADS)], axis=0)
    q2t[0:HEAD, :] = jnp.where(own_first, qa, qb).T
    q2t[HEAD:2 * HEAD, :] = jnp.where(own_first, qb, qa).T

    TN = (((0,), (0,)), ((), ()))

    for c in own_fills:
        c.wait()

    lane = lax.broadcasted_iota(jnp.int32, (RUN, ROWS), 1)
    keep = lax.broadcasted_iota(jnp.int32, (RUN, ROWS), 0) <= lane % RUN

    def triangle(kk, vv, qt, acc, total, top):
        s = jnp.dot(kk, qt, preferred_element_type=jnp.float32)
        s = jnp.where(keep, s, NEG)
        m = jnp.max(s, axis=0, keepdims=True)
        p = jnp.exp2(s * SCALE - m * SCALE)
        top[...] = m
        total[...] = jnp.sum(p.reshape(RUN // 8, 8, ROWS), axis=0)
        acc[...] = lax.dot_general(vv, p.astype(jnp.bfloat16), TN, preferred_element_type=jnp.float32)

    k0, k1, v0, v1 = (own_kv[i] for i in range(4))
    triangle(jnp.where(own_first, k0, k1), jnp.where(own_first, v0, v1), q2t[0:HEAD, :], acc_l, sum_l, max_l)
    triangle(jnp.where(own_first, k1, k0), jnp.where(own_first, v1, v0), q2t[HEAD:2 * HEAD, :], acc_h, sum_h, max_h)

    zero = jnp.zeros((16, HEAD), jnp.bfloat16)

    cat = functools.partial(jnp.concatenate, axis=0)

    def scores(f, i, r):
        kl, vl_, ka, kb, va, vb, low_f, high_f = ([] for _ in range(8))
        for j in range(8):
            s_z = jnp.where(f == 0, i, jnp.where(f == 1, (i % 2) * 4 + j // 2, j))
            s_x = jnp.where(f == 0, j // 2, jnp.where(f == 1, i // 2, i % 4))
            s_y = jnp.where(f == 2, i // 4, j % 2)
            s = cp_of(s_y, s_x, s_z)
            r0 = pos[s * TOK]
            r1 = pos[s * TOK + RUN]
            first = r0 < r1
            low = jnp.minimum(r0, r1) < own_low
            high = jnp.minimum(r0, r1) > own_low
            low_f.append(low)
            high_f.append(high)
            flags[j] = jnp.where(low, 1, 0)
            flags[8 + j] = jnp.where(high, 1, 0)
            for c in range(2):
                t0, t1, u0, u1 = (kv[f, c, i * 8 + j, n] for n in range(4))
                kl.append(jnp.where(first, t0, t1))
                vl_.append(jnp.where(first, u0, u1))
                ka.append(jnp.where(low, kl[-1], zero))
                va.append(jnp.where(low, vl_[-1], zero))
                kb.append(jnp.where(high, jnp.where(first, t1, t0), zero))
                vb.append(jnp.where(high, jnp.where(first, u1, u0), zero))
        vl[r % 2] = cat(vl_)
        v2[r % 2, :, 0:HEAD] = cat(va)
        v2[r % 2, :, HEAD:2 * HEAD] = cat(vb)
        k2 = jnp.concatenate([cat(ka), cat(kb)], axis=1)
        a = jnp.dot(cat(kl), q2t[HEAD:2 * HEAD, :], preferred_element_type=jnp.float32)
        b = jnp.dot(k2, q2t[...], preferred_element_type=jnp.float32)
        s1[...] = a
        s2[...] = b
        m_h = jnp.max(a.reshape(32, 8, ROWS), axis=0)
        m_l = jnp.full((8, ROWS), NEG, jnp.float32)
        for j in range(8):
            t = jnp.max(b[32 * j:32 * j + 32].reshape(4, 8, ROWS), axis=0)
            m_l = jnp.maximum(m_l, jnp.where(low_f[j], t, NEG))
            m_h = jnp.maximum(m_h, jnp.where(high_f[j], t, NEG))
        top_l[...] = m_l
        top_h[...] = m_h

    def weigh():
        old_l, old_h = max_l[...], max_h[...]
        new_l = jnp.maximum(old_l, jnp.max(top_l[...], axis=0, keepdims=True))
        new_h = jnp.maximum(old_h, jnp.max(top_h[...], axis=0, keepdims=True))
        f_l = jnp.exp2((old_l - new_l) * SCALE)
        f_h = jnp.exp2((old_h - new_h) * SCALE)
        max_l[...] = new_l
        max_h[...] = new_h
        fade_l[...] = f_l
        fade_h[...] = f_h
        at_l = jnp.broadcast_to(new_l * SCALE, (8, ROWS))
        at_h = jnp.broadcast_to(new_h * SCALE, (8, ROWS))
        t_h = sum_h[...] * f_h
        t_l = sum_l[...] * f_l
        for j in range(8):
            rows = slice(32 * j, 32 * j + 32)
            p = jnp.exp2(s1[rows, :].reshape(4, 8, ROWS) * SCALE - at_h[None])
            t_h = t_h + jnp.sum(p, axis=0)
            p1[rows, :] = p.reshape(32, ROWS).astype(jnp.bfloat16)
            low, high = flags[j] > 0, flags[8 + j] > 0
            m = jnp.where(low, at_l, jnp.where(high, at_h, -NEG))
            p = jnp.exp2(s2[rows, :].reshape(4, 8, ROWS) * SCALE - m[None])
            t = jnp.sum(p, axis=0)
            t_l = t_l + jnp.where(low, t, 0.0)
            t_h = t_h + jnp.where(high, t, 0.0)
            p2[rows, :] = p.reshape(32, ROWS).astype(jnp.bfloat16)
        sum_l[...] = t_l
        sum_h[...] = t_h

    def attend(r):
        r1 = lax.dot_general(vl[r % 2], p1[...], TN, preferred_element_type=jnp.float32)
        r2 = lax.dot_general(v2[r % 2], p2[...], TN, preferred_element_type=jnp.float32)
        acc_l[...] = acc_l[...] * fade_l[...] + r2[0:HEAD]
        acc_h[...] = acc_h[...] * fade_h[...] + (r1 + r2[HEAD:2 * HEAD])

    for ref in (s1, s2, top_l, top_h):
        ref[...] = jnp.full(ref.shape, NEG, jnp.float32)
    for ref in (p1, p2, vl, v2):
        ref[...] = jnp.zeros(ref.shape, jnp.bfloat16)
    fade_l[...] = jnp.ones((1, ROWS), jnp.float32)
    fade_h[...] = jnp.ones((1, ROWS), jnp.float32)
    for j in range(16):
        flags[j] = jnp.int32(1)

    codes = [chunk_code(GROUPS[g], half) for g, half, _ in ROUNDS]
    words = [codes[i] + 256 * codes[i + 1] + 65536 * codes[i + 2] for i in range(0, len(codes), 3)]

    def events_of(lo, hi, r):
        if hi - lo > 1:
            mid = (lo + hi) // 2
            pl.when(r < mid)(lambda: events_of(lo, mid, r))
            pl.when(r >= mid)(lambda: events_of(mid, hi, r))
            return
        g, _, events = ROUNDS[lo]
        for e in events:
            if e < 100:
                arrive(e).wait_recv()
            elif e < 200:
                gather(e - 100).start()
            else:
                share(e - 200, core).start()
        if g not in [other[0] for other in ROUNDS[:lo]]:
            share(g, 1 - core).wait_recv()

    def rounds(r, carry):
        events_of(0, len(ROUNDS), r)
        third = r // 3
        word = jnp.int32(0)
        for i, c in enumerate(words):
            word = jnp.where(third == i, c, word)
        code = jnp.where(r % 3 == 0, word % 256, jnp.where(r % 3 == 1, word // 256 % 256, word // 65536))
        f, k0, k1 = code // 64, code // 4 % 8, code % 4
        i = jnp.where(f == 0, (z + k0) % NZ,
                      jnp.where(f == 1, (x + k0) % NX * 2 + k1, (y + k1) % 2 * 4 + (x + k0) % NX))
        attend(r)
        weigh()
        scores(f, i, r)
        return carry

    lax.fori_loop(0, len(ROUNDS), rounds, 0)
    attend(len(ROUNDS))
    weigh()
    attend(len(ROUNDS) + 1)

    fin_l = acc_l[...] / jnp.sum(sum_l[...], axis=0, keepdims=True)
    fin_h = acc_h[...] / jnp.sum(sum_h[...], axis=0, keepdims=True)
    fin_a = jnp.where(own_first, fin_l, fin_h).T.astype(jnp.bfloat16)
    fin_b = jnp.where(own_first, fin_h, fin_l).T.astype(jnp.bfloat16)
    for h in range(HEADS):
        att[core, 0:RUN, h * HEAD:(h + 1) * HEAD] = fin_a[h * RUN:(h + 1) * RUN]
        att[core, RUN:TOK, h * HEAD:(h + 1) * HEAD] = fin_b[h * RUN:(h + 1) * RUN]
    att_copy = rcopy(att.at[core], att.at[core], att_sem.at[0], att_sem.at[1], partner)
    att_copy.start()
    w_own.wait()
    w_in.wait_recv()
    rcopy(att.at[1 - core], att.at[1 - core], att_sem.at[0], att_sem.at[1], partner).wait_recv()

    home = yh * 96
    far_sends, local_sends = [], []
    for j in range(NJ):
        w0 = wbuf[0:512, j * CW:(j + 1) * CW]
        w1 = wbuf[512:1024, j * CW:(j + 1) * CW]
        product = (jnp.dot(att[0], w0, preferred_element_type=jnp.float32)
                   + jnp.dot(att[1], w1, preferred_element_type=jnp.float32))
        pbuf[j] = product.astype(jnp.bfloat16)
        for e in range(2):
            rows = pl.ds(pl.multiple_of((1 - yh) * 96 + 48 * e, 48), 48)
            c = rcopy(pbuf.at[j, rows], rbuf.at[core, j], rs_send.at[2 * j + e], rs_recv.at[core, j], away_cores[e])
            c.start()
            far_sends.append(c)
        c = rcopy(pbuf.at[j, pl.ds(pl.multiple_of(home + 48 * (1 - core), 48), 48)], lbuf.at[j],
                  lo_send.at[j], lo_recv.at[j], partner)
        c.start()
        local_sends.append(c)

    mine = pl.multiple_of(core * HALF, HALF)
    theirs = pl.multiple_of((1 - core) * HALF, HALF)
    for j in range(NJ):
        rcopy(rbuf.at[core, j], rbuf.at[core, j], rs_send.at[0], rs_recv.at[core, j], partner).wait_recv()
        own = pbuf[j, pl.ds(pl.multiple_of(home + 48 * core, 48), 48), :]
        out_ref[:, pl.ds(mine + j * CW, CW)] = (
            own.astype(jnp.float32) + rbuf[core, j].astype(jnp.float32)).astype(jnp.bfloat16)
        local_sends[j].wait_recv()
        rcopy(rbuf.at[1 - core, j], rbuf.at[1 - core, j], rs_send.at[0], rs_recv.at[1 - core, j], partner).wait_recv()
        out_ref[:, pl.ds(theirs + j * CW, CW)] = (
            lbuf[j].astype(jnp.float32) + rbuf[1 - core, j].astype(jnp.float32)).astype(jnp.bfloat16)

    sends = [gather(i) for i in range(len(COPIES))] + [share(i, core) for i in range(len(GROUPS))]
    for c in sends + [w_far, att_copy] + far_sends + local_sends:
        c.wait_send()


def shards(queries, keys, values, positions, out_weight):
    dma = pltpu.SemaphoreType.DMA
    bf, f32 = jnp.bfloat16, jnp.float32
    return pl.pallas_call(
        kernel,
        out_shape=jax.ShapeDtypeStruct((48, NCOL), bf),
        in_specs=[pl.BlockSpec(memory_space=pltpu.HBM)] * 5,
        out_specs=pl.BlockSpec(memory_space=pltpu.VMEM),
        scratch_shapes=[
            pltpu.VMEM((3, 2, NCP, 4, 16, HEAD), bf),
            pltpu.VMEM((4, RUN, HEAD), bf),
            pltpu.VMEM((TOK, HEADS * HEAD), bf),
            pltpu.VMEM((2 * HEAD, ROWS), bf),
            pltpu.VMEM((HEAD, ROWS), f32),
            pltpu.VMEM((HEAD, ROWS), f32),
            pltpu.VMEM((8, ROWS), f32),
            pltpu.VMEM((8, ROWS), f32),
            pltpu.VMEM((1, ROWS), f32),
            pltpu.VMEM((1, ROWS), f32),
            pltpu.VMEM((256, ROWS), f32),
            pltpu.VMEM((256, ROWS), f32),
            pltpu.VMEM((256, ROWS), bf),
            pltpu.VMEM((256, ROWS), bf),
            pltpu.VMEM((2, 256, HEAD), bf),
            pltpu.VMEM((2, 256, 2 * HEAD), bf),
            pltpu.VMEM((8, ROWS), f32),
            pltpu.VMEM((8, ROWS), f32),
            pltpu.VMEM((1, ROWS), f32),
            pltpu.VMEM((1, ROWS), f32),
            pltpu.VMEM((2, TOK, 512), bf),
            pltpu.VMEM((1024, HALF), bf),
            pltpu.VMEM((NJ, TOK, CW), bf),
            pltpu.VMEM((2, NJ, 48, CW), bf),
            pltpu.VMEM((NJ, 48, CW), bf),
            pltpu.SMEM((NCP * TOK,), jnp.int32),
            pltpu.SMEM((16,), jnp.int32),
            dma((16,)),
            dma((2,)),
            dma((3,)),
            dma((len(COPIES),)),
            dma((len(COPIES),)),
            dma((len(GROUPS),)),
            dma((len(GROUPS),)),
            dma((2,)),
            dma((2 * NJ,)),
            dma((2, NJ)),
            dma((NJ,)),
            dma((NJ,)),
        ],
        compiler_params=pltpu.CompilerParams(collective_id=0, has_side_effects=True,
                                             vmem_limit_bytes=48 * 1024 * 1024),
    )(*(pltpu.with_memory_space_constraint(a, pltpu.HBM) for a in (queries, keys, values, positions)), out_weight)


def solution(mesh):
    in_specs = (P("cp", "tp"), P("cp", None), P("cp", None), P(), P("tp", None))
    out_specs = P(("cp", "tp"), None)
    return jax.shard_map(shards, mesh=mesh, in_specs=in_specs, out_specs=out_specs, check_vma=False)
```

```python
import functools
import math

import jax
import jax.numpy as jnp
from jax import lax
from jax.experimental import pallas as pl
from jax.experimental.pallas import tpu as pltpu
from jax.sharding import PartitionSpec as P

MESH = pl.DeviceIdType.MESH
HEAD = 128
GROUP = 8
NY, NX, NZ = 2, 4, 8
NCP = NY * NX * NZ
RUN = 96
TOK = 192
HEADS = 4
ROWS = RUN * HEADS
NCOL = 8192
HALF = NCOL // 2
NJ = 8
CW = HALF // NJ
SCALE = HEAD ** (-0.5) * math.log2(math.e)
NEG = -1e30


COPIES = (
    (0, 0, 0, 1, 2, 1), (6, -2, 0, 1, 1, 2), (6, 2, 0, 1, 1, -2), (3, 0, 0, 1, 2, 1), (6, -1, 0, 1, 1, 1),
    (6, 1, 0, 1, 1, -1), (1, 2, 0, 2, 0, 2), (1, -1, 0, 2, 0, 1), (1, 1, 0, 2, 0, -1), (4, -2, 0, 2, 1, 2),
    (4, 2, 0, 2, 1, -2), (4, -1, 0, 2, 1, 1), (4, 1, 0, 2, 1, -1), (5, -1, 0, 2, 0, 1), (5, 1, 0, 2, 0, -1),
    (6, -4, 0, 1, 1, 2), (6, -3, 0, 1, 1, 1), (6, 3, 0, 1, 1, -1), (2, -1, 0, 4, 1, 1), (2, 1, 1, 4, 1, -1),
    (2, 1, 0, 4, 1, -1), (2, -1, 1, 4, 1, 1), (5, 1, -1, 2, 0, -1), (5, -1, -1, 2, 0, 1), (5, 1, 1, 2, 0, -1),
    (5, -1, 1, 2, 0, 1), (4, -4, 0, 2, 1, 2), (4, -3, 0, 2, 1, 1), (5, -1, -2, 2, 0, 1), (5, 1, -2, 2, 0, -1),
    (4, 3, 0, 2, 1, -1), (5, -1, 2, 2, 0, 1), (5, 1, 2, 2, 0, -1), (5, 2, 0, 2, 0, 1), (7, -1, 0, 8, 0, 1),
    (7, 1, 0, 8, 0, -1), (8, 0, 0, 8, 2, 1), (5, 2, -1, 2, 0, -1), (2, -2, 0, 4, 1, 1), (2, 2, 1, 4, 1, -1),
    (5, 2, 1, 2, 0, -1), (5, 2, -2, 2, 0, 1), (2, -2, 1, 4, 1, 1), (2, 2, 0, 4, 1, -1), (5, 2, 2, 2, 0, 1),
    (5, 1, 3, 2, 0, -1), (5, -1, 3, 2, 0, 1), (5, 1, -3, 2, 0, -1), (5, -1, -3, 2, 0, 1), (5, -1, -4, 2, 0, 1),
    (5, 1, -4, 2, 0, -1), (7, 2, 1, 4, 0, -1), (8, 1, 0, 8, 2, 1), (7, 2, 0, 4, 0, 1), (8, -1, 0, 8, 2, 1),
    (2, -3, 0, 4, 1, 1), (2, 3, 1, 4, 1, -1), (2, -3, 1, 4, 1, 1), (5, 2, 3, 2, 0, -1), (2, 3, 0, 4, 1, -1),
    (5, 2, -3, 2, 0, -1), (5, 2, -4, 2, 0, 1), (8, 2, 0, 8, 2, 1), (2, -4, 0, 4, 1, 1), (2, 4, 1, 4, 1, -1),
)
GROUPS = (
    (0, 0, 0), (2, 0, 0), (0, -1, 0), (0, 1, 0), (2, 0, 1), (1, 0, 0), (2, 1, 0), (2, -1, 0), (0, -2, 0), (0, 2, 0),
    (1, 1, 0), (1, -1, 0), (2, 2, 0), (2, 1, 1), (0, -3, 0), (0, 3, 0), (1, 2, 0), (2, -1, 1), (0, -4, 0),
    (2, 2, 1),
)
FIRST = 6
ROUNDS = (
    (0, 0, (0, 106, 107, 108, 3, 109, 110, 111, 112, 113, 114, 4, 5, 1, 115, 116, 2, 117, 8, 14, 7, 6, 118, 119, 120, 121, 200, 11, 122, 123, 12, 124, 125, 9, 126, 127, 128, 129, 10, 130, 131, 132, 13, 133, 17, 16, 15, 134, 135, 136, 201)),
    (1, 0, ()),
    (2, 0, (22, 137, 23, 18, 138, 19, 139, 24, 140, 25, 29, 28, 141, 21, 142, 202, 20, 143, 203, 32, 31, 144, 30, 145, 146, 33)),
    (3, 0, (36, 204, 27, 147, 148, 26, 149, 150, 205)),
    (4, 0, (35, 151, 152, 206, 37, 34, 153, 154, 207, 38, 155, 39, 156)), (5, 0, (40, 41)),
    (5, 1, (44, 42, 157, 208, 45, 158, 43, 159, 209, 46)), (6, 0, ()), (7, 0, (47, 160, 48)),
    (8, 0, (50, 210, 49, 161, 211)), (9, 0, ()), (10, 0, (51, 53, 162, 212, 55, 163, 56, 164)),
    (10, 1, (52, 213, 58)), (11, 0, (57, 214, 59, 215)), (11, 1, (60,)), (12, 0, (61, 216)), (13, 0, (54, 217)),
    (14, 0, ()), (15, 0, ()), (16, 0, (63, 64, 218)), (16, 1, ()), (17, 0, (62, 219)), (18, 0, ()), (19, 0, ()),
)


def place(copy, x, z, y):
    kind, k0, k1, n = copy[:4]
    at_x, at_z, at_y = (x + k0 + NX) % NX, (z + k0 + NZ) % NZ, 1 - y
    slot = (
        z * 8 + x * 2 + at_y,
        z * 8 + at_x * 2,
        at_z * 8 + k1 * 4,
        x * 16 + z * 2 + at_y,
        x * 16 + at_z * 2,
        at_x * 16 + (z + k1 + NZ) % NZ * 2,
        y * 32 + x * 8 + at_z,
        y * 32 + at_x * 8 + k1 * 4,
        at_y * 32 + at_x * 8,
    )[kind]
    return kind // 3, slot, n


def group_place(group, x, z, y):
    f, k0, k1 = group
    at_x = (x + k0 + NX) % NX
    slot = ((z + k0 + NZ) % NZ * 8, at_x * 16, (y + k1) % 2 * 32 + at_x * 8)[f]
    return f, slot, 16 if f == 1 else 8


def chunk_code(group, half):
    f, k0, k1 = group
    return f * 64 + k0 % 8 * 4 + (k1 if f == 2 else half)


def kernel(q_ref, k_ref, v_ref, pos_ref, w_ref, out_ref,
           kv, own_kv, qv, q2t, acc_l, acc_h, sum_l, sum_h, max_l, max_h,
           s1, s2, p1, p2, vl, v2, top_l, top_h, fade_l, fade_h,
           att, wbuf, pbuf, rbuf, lbuf, pos, flags,
           fill_sem, in_sem, w_sem, ag_send, ag_recv, dd_send, dd_recv,
           att_sem, rs_send, rs_recv, lo_send, lo_recv):
    cp = lax.axis_index("cp")
    tp = lax.axis_index("tp")
    core = tp % 2
    yh = tp // 2
    z = cp % NZ
    x = (cp // NZ) % NX
    y = cp // (NZ * NX)

    def cp_of(yy, xx, zz):
        return (yy * NX + xx) * NZ + zz

    partner = dict(cp=cp, tp=yh * 2 + 1 - core)

    def zz(k):
        return (z + k + NZ) % NZ

    def xx(k):
        return (x + k + NX) % NX

    def at_z(k):
        return dict(cp=cp_of(y, x, zz(k)), tp=tp)

    def at_x(k):
        return dict(cp=cp_of(y, xx(k), z), tp=tp)

    flip = dict(cp=cp_of(1 - y, x, z), tp=tp)
    away_cores = [dict(cp=cp, tp=(1 - yh) * 2 + e) for e in (0, 1)]

    q_copy = pltpu.make_async_copy(q_ref, qv, in_sem.at[0])
    q_copy.start()
    pos_copy = pltpu.make_async_copy(pos_ref, pos, in_sem.at[1])
    pos_copy.start()
    slot_a = z * 8 + x * 2 + y
    slot_b = x * 16 + z * 2 + y
    slot_d = y * 32 + x * 8 + z
    own_slots = (slot_a, slot_b, slot_d)
    fills = []
    cols = pl.ds(pl.multiple_of(yh * HEAD, HEAD), HEAD)
    for f in range(3):
        for h in range(2):
            for src, kind in ((k_ref, 0), (v_ref, 2)):
                rows = pl.ds(pl.multiple_of(h * RUN + 32 * f + 16 * core, 16), 16)
                fills.append(pltpu.make_async_copy(
                    src.at[rows, cols], kv.at[f, core, own_slots[f], kind + h], fill_sem.at[len(fills)]))
    own_fills = []
    for h in range(2):
        for src, kind in ((k_ref, 0), (v_ref, 2)):
            own_fills.append(pltpu.make_async_copy(
                src.at[pl.ds(h * RUN, RUN), cols], own_kv.at[kind + h], fill_sem.at[12 + len(own_fills)]))
    for c in fills + own_fills:
        c.start()

    my_rows = pl.ds(pl.multiple_of(core * 512, 512), 512)
    w_own = pltpu.make_async_copy(
        w_ref.at[:, pl.ds(pl.multiple_of(core * HALF, HALF), HALF)], wbuf.at[my_rows], w_sem.at[0])
    w_own.start()

    barrier = pltpu.get_barrier_semaphore()
    x_steps = sorted({sign * c[5] % NX for c in COPIES if c[4] == 0 for sign in (1, -1)})
    z_steps = sorted({sign * c[5] % NZ for c in COPIES if c[4] == 1 for sign in (1, -1)})
    peers = [at_z(k) for k in z_steps] + [at_x(k) for k in x_steps] + [partner, flip] + away_cores
    for p in peers:
        pl.semaphore_signal(barrier, inc=1, device_id=p, device_id_type=MESH)
    pl.semaphore_wait(barrier, len(peers))
    for c in fills:
        c.wait()

    def rcopy(src, dst, ssem, rsem, dev):
        return pltpu.make_async_remote_copy(src_ref=src, dst_ref=dst, send_sem=ssem, recv_sem=rsem,
                                            device_id=dev, device_id_type=MESH)

    def part(owner, where):
        f, slot, n = where
        return kv.at[f, owner, pl.ds(slot, n)]

    def gather(i):
        axis, steps = COPIES[i][4:]
        dev = (at_x, at_z, lambda k: flip)[axis](steps)
        where = place(COPIES[i], xx(steps) if axis == 0 else x, zz(steps) if axis == 1 else z, 1 - y if axis == 2 else y)
        ref = part(core, where)
        return rcopy(ref, ref, ag_send.at[i], ag_recv.at[i], dev)

    def arrive(i):
        ref = part(core, place(COPIES[i], x, z, y))
        return rcopy(ref, ref, ag_send.at[i], ag_recv.at[i], partner)

    def share(i, owner):
        ref = part(owner, group_place(GROUPS[i], x, z, y))
        return rcopy(ref, ref, dd_send.at[i], dd_recv.at[i], partner)

    for i in range(FIRST):
        gather(i).start()

    w_far = rcopy(w_ref.at[:, pl.ds(pl.multiple_of((1 - core) * HALF, HALF), HALF)], wbuf.at[my_rows],
                  w_sem.at[1], w_sem.at[2], partner)
    w_far.start()
    other_rows = pl.ds(pl.multiple_of((1 - core) * 512, 512), 512)
    w_in = rcopy(w_ref.at[:, pl.ds(0, HALF)], wbuf.at[other_rows], w_sem.at[1], w_sem.at[2], partner)

    q_copy.wait()
    pos_copy.wait()
    own0 = pos[cp * TOK]
    own1 = pos[cp * TOK + RUN]
    own_first = own0 < own1
    own_low = jnp.minimum(own0, own1)

    qa = jnp.concatenate([qv[0:RUN, h * HEAD:(h + 1) * HEAD] for h in range(HEADS)], axis=0)
    qb = jnp.concatenate([qv[RUN:TOK, h * HEAD:(h + 1) * HEAD] for h in range(HEADS)], axis=0)
    q2t[0:HEAD, :] = jnp.where(own_first, qa, qb).T
    q2t[HEAD:2 * HEAD, :] = jnp.where(own_first, qb, qa).T

    TN = (((0,), (0,)), ((), ()))

    for c in own_fills:
        c.wait()

    lane = lax.broadcasted_iota(jnp.int32, (RUN, ROWS), 1)
    keep = lax.broadcasted_iota(jnp.int32, (RUN, ROWS), 0) <= lane % RUN

    def triangle(kk, vv, qt, acc, total, top):
        s = jnp.dot(kk, qt, preferred_element_type=jnp.float32)
        s = jnp.where(keep, s, NEG)
        m = jnp.max(s, axis=0, keepdims=True)
        p = jnp.exp2(s * SCALE - m * SCALE)
        top[...] = m
        total[...] = jnp.sum(p.reshape(RUN // 8, 8, ROWS), axis=0)
        acc[...] = lax.dot_general(vv, p.astype(jnp.bfloat16), TN, preferred_element_type=jnp.float32)

    k0, k1, v0, v1 = (own_kv[i] for i in range(4))
    triangle(jnp.where(own_first, k0, k1), jnp.where(own_first, v0, v1), q2t[0:HEAD, :], acc_l, sum_l, max_l)
    triangle(jnp.where(own_first, k1, k0), jnp.where(own_first, v1, v0), q2t[HEAD:2 * HEAD, :], acc_h, sum_h, max_h)

    zero = jnp.zeros((16, HEAD), jnp.bfloat16)

    cat = functools.partial(jnp.concatenate, axis=0)

    def scores(f, i, r):
        kl, vl_, ka, kb, va, vb, low_f, high_f = ([] for _ in range(8))
        for j in range(8):
            s_z = jnp.where(f == 0, i, jnp.where(f == 1, (i % 2) * 4 + j // 2, j))
            s_x = jnp.where(f == 0, j // 2, jnp.where(f == 1, i // 2, i % 4))
            s_y = jnp.where(f == 2, i // 4, j % 2)
            s = cp_of(s_y, s_x, s_z)
            r0 = pos[s * TOK]
            r1 = pos[s * TOK + RUN]
            first = r0 < r1
            low = jnp.minimum(r0, r1) < own_low
            high = jnp.minimum(r0, r1) > own_low
            low_f.append(low)
            high_f.append(high)
            flags[j] = jnp.where(low, 1, 0)
            flags[8 + j] = jnp.where(high, 1, 0)
            for c in range(2):
                t0, t1, u0, u1 = (kv[f, c, i * 8 + j, n] for n in range(4))
                kl.append(jnp.where(first, t0, t1))
                vl_.append(jnp.where(first, u0, u1))
                ka.append(jnp.where(low, kl[-1], zero))
                va.append(jnp.where(low, vl_[-1], zero))
                kb.append(jnp.where(high, jnp.where(first, t1, t0), zero))
                vb.append(jnp.where(high, jnp.where(first, u1, u0), zero))
        vl[r % 2] = cat(vl_)
        v2[r % 2, :, 0:HEAD] = cat(va)
        v2[r % 2, :, HEAD:2 * HEAD] = cat(vb)
        k2 = jnp.concatenate([cat(ka), cat(kb)], axis=1)
        a = jnp.dot(cat(kl), q2t[HEAD:2 * HEAD, :], preferred_element_type=jnp.float32)
        b = jnp.dot(k2, q2t[...], preferred_element_type=jnp.float32)
        s1[...] = a
        s2[...] = b
        m_h = jnp.max(a.reshape(32, 8, ROWS), axis=0)
        m_l = jnp.full((8, ROWS), NEG, jnp.float32)
        for j in range(8):
            t = jnp.max(b[32 * j:32 * j + 32].reshape(4, 8, ROWS), axis=0)
            m_l = jnp.maximum(m_l, jnp.where(low_f[j], t, NEG))
            m_h = jnp.maximum(m_h, jnp.where(high_f[j], t, NEG))
        top_l[...] = m_l
        top_h[...] = m_h

    def weigh():
        old_l, old_h = max_l[...], max_h[...]
        new_l = jnp.maximum(old_l, jnp.max(top_l[...], axis=0, keepdims=True))
        new_h = jnp.maximum(old_h, jnp.max(top_h[...], axis=0, keepdims=True))
        f_l = jnp.exp2((old_l - new_l) * SCALE)
        f_h = jnp.exp2((old_h - new_h) * SCALE)
        max_l[...] = new_l
        max_h[...] = new_h
        fade_l[...] = f_l
        fade_h[...] = f_h
        at_l = jnp.broadcast_to(new_l * SCALE, (8, ROWS))
        at_h = jnp.broadcast_to(new_h * SCALE, (8, ROWS))
        t_h = sum_h[...] * f_h
        t_l = sum_l[...] * f_l
        for j in range(8):
            rows = slice(32 * j, 32 * j + 32)
            p = jnp.exp2(s1[rows, :].reshape(4, 8, ROWS) * SCALE - at_h[None])
            t_h = t_h + jnp.sum(p, axis=0)
            p1[rows, :] = p.reshape(32, ROWS).astype(jnp.bfloat16)
            low, high = flags[j] > 0, flags[8 + j] > 0
            m = jnp.where(low, at_l, jnp.where(high, at_h, -NEG))
            p = jnp.exp2(s2[rows, :].reshape(4, 8, ROWS) * SCALE - m[None])
            t = jnp.sum(p, axis=0)
            t_l = t_l + jnp.where(low, t, 0.0)
            t_h = t_h + jnp.where(high, t, 0.0)
            p2[rows, :] = p.reshape(32, ROWS).astype(jnp.bfloat16)
        sum_l[...] = t_l
        sum_h[...] = t_h

    def attend(r):
        r1 = lax.dot_general(vl[r % 2], p1[...], TN, preferred_element_type=jnp.float32)
        r2 = lax.dot_general(v2[r % 2], p2[...], TN, preferred_element_type=jnp.float32)
        acc_l[...] = acc_l[...] * fade_l[...] + r2[0:HEAD]
        acc_h[...] = acc_h[...] * fade_h[...] + (r1 + r2[HEAD:2 * HEAD])

    for ref in (s1, s2, top_l, top_h):
        ref[...] = jnp.full(ref.shape, NEG, jnp.float32)
    for ref in (p1, p2, vl, v2):
        ref[...] = jnp.zeros(ref.shape, jnp.bfloat16)
    fade_l[...] = jnp.ones((1, ROWS), jnp.float32)
    fade_h[...] = jnp.ones((1, ROWS), jnp.float32)
    for j in range(16):
        flags[j] = jnp.int32(1)

    codes = [chunk_code(GROUPS[g], half) for g, half, _ in ROUNDS]
    words = [codes[i] + 256 * codes[i + 1] + 65536 * codes[i + 2] for i in range(0, len(codes), 3)]

    def events_of(lo, hi, r):
        if hi - lo > 1:
            mid = (lo + hi) // 2
            pl.when(r < mid)(lambda: events_of(lo, mid, r))
            pl.when(r >= mid)(lambda: events_of(mid, hi, r))
            return
        g, _, events = ROUNDS[lo]
        for e in events:
            if e < 100:
                arrive(e).wait_recv()
            elif e < 200:
                gather(e - 100).start()
            else:
                share(e - 200, core).start()
        if g not in [other[0] for other in ROUNDS[:lo]]:
            share(g, 1 - core).wait_recv()

    def rounds(r, carry):
        events_of(0, len(ROUNDS), r)
        third = r // 3
        word = jnp.int32(0)
        for i, c in enumerate(words):
            word = jnp.where(third == i, c, word)
        code = jnp.where(r % 3 == 0, word % 256, jnp.where(r % 3 == 1, word // 256 % 256, word // 65536))
        f, k0, k1 = code // 64, code // 4 % 8, code % 4
        i = jnp.where(f == 0, (z + k0) % NZ,
                      jnp.where(f == 1, (x + k0) % NX * 2 + k1, (y + k1) % 2 * 4 + (x + k0) % NX))
        attend(r)
        weigh()
        scores(f, i, r)
        return carry

    lax.fori_loop(0, len(ROUNDS), rounds, 0)
    attend(len(ROUNDS))
    weigh()
    attend(len(ROUNDS) + 1)

    fin_l = acc_l[...] / jnp.sum(sum_l[...], axis=0, keepdims=True)
    fin_h = acc_h[...] / jnp.sum(sum_h[...], axis=0, keepdims=True)
    fin_a = jnp.where(own_first, fin_l, fin_h).T.astype(jnp.bfloat16)
    fin_b = jnp.where(own_first, fin_h, fin_l).T.astype(jnp.bfloat16)
    for h in range(HEADS):
        att[core, 0:RUN, h * HEAD:(h + 1) * HEAD] = fin_a[h * RUN:(h + 1) * RUN]
        att[core, RUN:TOK, h * HEAD:(h + 1) * HEAD] = fin_b[h * RUN:(h + 1) * RUN]
    att_copy = rcopy(att.at[core], att.at[core], att_sem.at[0], att_sem.at[1], partner)
    att_copy.start()
    w_own.wait()
    w_in.wait_recv()
    rcopy(att.at[1 - core], att.at[1 - core], att_sem.at[0], att_sem.at[1], partner).wait_recv()

    home = yh * 96
    far_sends, local_sends = [], []
    for j in range(NJ):
        w0 = wbuf[0:512, j * CW:(j + 1) * CW]
        w1 = wbuf[512:1024, j * CW:(j + 1) * CW]
        product = (jnp.dot(att[0], w0, preferred_element_type=jnp.float32)
                   + jnp.dot(att[1], w1, preferred_element_type=jnp.float32))
        pbuf[j] = product.astype(jnp.bfloat16)
        for e in range(2):
            rows = pl.ds(pl.multiple_of((1 - yh) * 96 + 48 * e, 48), 48)
            c = rcopy(pbuf.at[j, rows], rbuf.at[core, j], rs_send.at[2 * j + e], rs_recv.at[core, j], away_cores[e])
            c.start()
            far_sends.append(c)
        c = rcopy(pbuf.at[j, pl.ds(pl.multiple_of(home + 48 * (1 - core), 48), 48)], lbuf.at[j],
                  lo_send.at[j], lo_recv.at[j], partner)
        c.start()
        local_sends.append(c)

    mine = pl.multiple_of(core * HALF, HALF)
    theirs = pl.multiple_of((1 - core) * HALF, HALF)
    for j in range(NJ):
        rcopy(rbuf.at[core, j], rbuf.at[core, j], rs_send.at[0], rs_recv.at[core, j], partner).wait_recv()
        own = pbuf[j, pl.ds(pl.multiple_of(home + 48 * core, 48), 48), :]
        out_ref[:, pl.ds(mine + j * CW, CW)] = (
            own.astype(jnp.float32) + rbuf[core, j].astype(jnp.float32)).astype(jnp.bfloat16)
        local_sends[j].wait_recv()
        rcopy(rbuf.at[1 - core, j], rbuf.at[1 - core, j], rs_send.at[0], rs_recv.at[1 - core, j], partner).wait_recv()
        out_ref[:, pl.ds(theirs + j * CW, CW)] = (
            lbuf[j].astype(jnp.float32) + rbuf[1 - core, j].astype(jnp.float32)).astype(jnp.bfloat16)

    sends = [gather(i) for i in range(len(COPIES))] + [share(i, core) for i in range(len(GROUPS))]
    for c in sends + [w_far, att_copy] + far_sends + local_sends:
        c.wait_send()


def shards(queries, keys, values, positions, out_weight):
    dma = pltpu.SemaphoreType.DMA
    bf, f32 = jnp.bfloat16, jnp.float32
    return pl.pallas_call(
        kernel,
        out_shape=jax.ShapeDtypeStruct((48, NCOL), bf),
        in_specs=[pl.BlockSpec(memory_space=pltpu.HBM)] * 5,
        out_specs=pl.BlockSpec(memory_space=pltpu.VMEM),
        scratch_shapes=[
            pltpu.VMEM((3, 2, NCP, 4, 16, HEAD), bf),
            pltpu.VMEM((4, RUN, HEAD), bf),
            pltpu.VMEM((TOK, HEADS * HEAD), bf),
            pltpu.VMEM((2 * HEAD, ROWS), bf),
            pltpu.VMEM((HEAD, ROWS), f32),
            pltpu.VMEM((HEAD, ROWS), f32),
            pltpu.VMEM((8, ROWS), f32),
            pltpu.VMEM((8, ROWS), f32),
            pltpu.VMEM((1, ROWS), f32),
            pltpu.VMEM((1, ROWS), f32),
            pltpu.VMEM((256, ROWS), f32),
            pltpu.VMEM((256, ROWS), f32),
            pltpu.VMEM((256, ROWS), bf),
            pltpu.VMEM((256, ROWS), bf),
            pltpu.VMEM((2, 256, HEAD), bf),
            pltpu.VMEM((2, 256, 2 * HEAD), bf),
            pltpu.VMEM((8, ROWS), f32),
            pltpu.VMEM((8, ROWS), f32),
            pltpu.VMEM((1, ROWS), f32),
            pltpu.VMEM((1, ROWS), f32),
            pltpu.VMEM((2, TOK, 512), bf),
            pltpu.VMEM((1024, HALF), bf),
            pltpu.VMEM((NJ, TOK, CW), bf),
            pltpu.VMEM((2, NJ, 48, CW), bf),
            pltpu.VMEM((NJ, 48, CW), bf),
            pltpu.SMEM((NCP * TOK,), jnp.int32),
            pltpu.SMEM((16,), jnp.int32),
            dma((16,)),
            dma((2,)),
            dma((3,)),
            dma((len(COPIES),)),
            dma((len(COPIES),)),
            dma((len(GROUPS),)),
            dma((len(GROUPS),)),
            dma((2,)),
            dma((2 * NJ,)),
            dma((2, NJ)),
            dma((NJ,)),
            dma((NJ,)),
        ],
        compiler_params=pltpu.CompilerParams(collective_id=0, has_side_effects=True,
                                             vmem_limit_bytes=48 * 1024 * 1024),
    )(*(pltpu.with_memory_space_constraint(a, pltpu.HBM) for a in (queries, keys, values, positions)), out_weight)


def solution(mesh):
    in_specs = (P("cp", "tp"), P("cp", None), P("cp", None), P(), P("tp", None))
    out_specs = P(("cp", "tp"), None)
    return jax.shard_map(shards, mesh=mesh, in_specs=in_specs, out_specs=out_specs, check_vma=False)
```
